32 devices in a mesh: gz: 8 (over z, x), gy: 4 (over y, core).
Axes of the slice: x: 2, y: 2, z: 4, core: 2. Of those that a mesh axis runs over, the one named last changes fastest.
Arguments:
- source_first: float32 [64, 32, 16, 128], P('gz', 'gy'), may hold values from -6 to 6
- source_second: float32 [32, 16, 16, 128], P('gz', 'gy'), may hold values from -6 to 6
- source_third: float32 [16, 8, 16, 128], P('gz', 'gy'), may hold values from -6 to 6
- source_fourth: float32 [8, 4, 16, 128], P('gz', 'gy'), may hold values from -6 to 6
- guess_first: float32 [64, 32, 16, 128], P('gz', 'gy'), may hold values from -6 to 6
- guess_second: float32 [32, 16, 16, 128], P('gz', 'gy'), may hold values from -6 to 6
- guess_third: float32 [16, 8, 16, 128], P('gz', 'gy'), may hold values from -6 to 6
- guess_fourth: float32 [8, 4, 16, 128], P('gz', 'gy'), may hold values from -6 to 6
- shift_first: float32 [64, 32, 128], P('gz', 'gy'), may hold values from 0.2 to 2
- shift_second: float32 [32, 16, 128], P('gz', 'gy'), may hold values from 0.2 to 2
- shift_third: float32 [16, 8, 128], P('gz', 'gy'), may hold values from 0.2 to 2
- shift_fourth: float32 [8, 4, 128], P('gz', 'gy'), may hold values from 0.2 to 2
- blocks_first: bfloat16 [64, 32, 2, 128, 128], P('gz', 'gy'), may hold values from -0.375 to 0.375
- blocks_second: bfloat16 [32, 16, 2, 128, 128], P('gz', 'gy'), may hold values from -0.375 to 0.375
- blocks_third: bfloat16 [16, 8, 2, 128, 128], P('gz', 'gy'), may hold values from -0.375 to 0.375
- links_first: int32 [64, 32, 2], P('gz', 'gy'), may hold values from 0 to 511, as said below
- links_second: int32 [32, 16, 2], P('gz', 'gy'), may hold values from 0 to 127, as said below
- links_third: int32 [16, 8, 2], P('gz', 'gy'), may hold values from 0 to 31, as said below
Outputs:
- smooth_first: float32 [64, 32, 16, 128], P('gz', 'gy')
- smooth_second: float32 [32, 16, 16, 128], P('gz', 'gy')
- smooth_third: float32 [16, 8, 16, 128], P('gz', 'gy')
- smooth_fourth: float32 [8, 4, 16, 128], P('gz', 'gy')
The draws below stay inside these ranges and needn't reach their ends.
Inputs may be any that keep to these rules, and one draw needn't show every extreme that they name: `links_first`: entry k of fine cell (i, j) names coarse column x * 16 + y with x within one of i // 2 and y within one of j // 2, both periodic on the coarse grid. `links_second`: entry k of cell (i, j) names coarse column x * 8 + y with x within one of i // 2 and y within one of j // 2, both periodic on the coarse grid. `links_third`: entry k of cell (i, j) names coarse column x * 4 + y with x within one of i // 2 and y within one of j // 2, both periodic on the coarse grid.
All inputs are finite; a program needn't handle non-finite values.
Results may differ from the reference program's by a relative error of at most 0.0005.
Values may be sent and summed in bfloat16 or wider, within the bound.
A program may use at most 256 MiB of HBM per device.

```python
import math
import jax
import jax.numpy as jnp
from jax import lax

LINE = 128
SIDES = 16
LINKS = 2
DEGREE = 3
NX0 = 64
NY0 = 32
NX1 = 32
NY1 = 16
NX2 = 16
NY2 = 8
NX3 = 8
NY3 = 4


def column_links(key, fine_rows, fine_cols, coarse_rows, coarse_cols):
    offsets = jax.random.randint(jax.random.fold_in(key, 17), (fine_rows, fine_cols, LINKS, 2), -1, 2)
    row_index = (jnp.arange(fine_rows, dtype=jnp.int32) // 2)[:, None, None]
    col_index = (jnp.arange(fine_cols, dtype=jnp.int32) // 2)[None, :, None]
    coarse_row = (row_index + offsets[..., 0]) % coarse_rows
    coarse_col = (col_index + offsets[..., 1]) % coarse_cols
    return (coarse_row * coarse_cols + coarse_col).astype(jnp.int32)


def draw_links_first(key, part):
    return column_links(key, NX0, NY0, NX1, NY1)


def draw_links_second(key, part):
    return column_links(key, NX1, NY1, NX2, NY2)


def draw_links_third(key, part):
    return column_links(key, NX2, NY2, NX3, NY3)


def level_of(own_key, extent, shards, low, high):
    loudness = 1.0
    for position, shards_of in shards:
        draws = jax.random.uniform(jax.random.fold_in(jax.random.fold_in(own_key, 6), position), (shards_of,), jnp.float32, low / len(shards), high / len(shards))
        loudness = loudness * jnp.repeat(jnp.exp(draws), extent[position] // shards_of).reshape((-1,) + (1,) * (len(extent) - 1 - position))
    return loudness


def centred(key, shape, width, most, shards=(), held_as=jnp.bfloat16):
    factor_of = level_of(key, shape, shards, -0.22, 0.18) if shards else 1.0
    array = jax.random.normal(key, shape, jnp.float32) * width * factor_of
    return jnp.minimum(jnp.maximum(array, -most), most).astype(held_as)


def setup_inputs(seed: int = 0) -> dict:
    key_list = jax.random.split(jax.random.key(seed), 19)
    source_first = centred(key_list[0], (NX0, NY0, SIDES, LINE), 1.0, 6.0, ((0, 8), (1, 4)), jnp.float32)
    source_second = centred(key_list[1], (NX1, NY1, SIDES, LINE), 1.0, 6.0, ((0, 8), (1, 4)), jnp.float32)
    source_third = centred(key_list[2], (NX2, NY2, SIDES, LINE), 1.0, 6.0, ((0, 8), (1, 4)), jnp.float32)
    source_fourth = centred(key_list[3], (NX3, NY3, SIDES, LINE), 1.0, 6.0, ((0, 8), (1, 4)), jnp.float32)
    guess_first = centred(key_list[4], (NX0, NY0, SIDES, LINE), 1.0, 6.0, ((0, 8), (1, 4)), jnp.float32)
    guess_second = centred(key_list[5], (NX1, NY1, SIDES, LINE), 1.0, 6.0, ((0, 8), (1, 4)), jnp.float32)
    guess_third = centred(key_list[6], (NX2, NY2, SIDES, LINE), 1.0, 6.0, ((0, 8), (1, 4)), jnp.float32)
    guess_fourth = centred(key_list[7], (NX3, NY3, SIDES, LINE), 1.0, 6.0, ((0, 8), (1, 4)), jnp.float32)
    shift_first = jnp.clip(jnp.exp(math.log(2.0) - 2.3025851 * jax.random.uniform(key_list[8], (NX0, NY0, LINE), jnp.float32) ** level_of(key_list[8], (NX0, NY0, LINE), ((0, 8), (1, 4)), -0.2, 0.2)), 0.2, 2.0)
    shift_second = jnp.clip(jnp.exp(math.log(2.0) - 2.3025851 * jax.random.uniform(key_list[9], (NX1, NY1, LINE), jnp.float32) ** level_of(key_list[9], (NX1, NY1, LINE), ((0, 8), (1, 4)), -0.2, 0.2)), 0.2, 2.0)
    shift_third = jnp.clip(jnp.exp(math.log(2.0) - 2.3025851 * jax.random.uniform(key_list[10], (NX2, NY2, LINE), jnp.float32) ** level_of(key_list[10], (NX2, NY2, LINE), ((0, 8), (1, 4)), -0.2, 0.2)), 0.2, 2.0)
    shift_fourth = jnp.clip(jnp.exp(math.log(2.0) - 2.3025851 * jax.random.uniform(key_list[11], (NX3, NY3, LINE), jnp.float32) ** level_of(key_list[11], (NX3, NY3, LINE), ((0, 8), (1, 4)), -0.2, 0.2)), 0.2, 2.0)
    blocks_first = centred(key_list[12], (NX0, NY0, LINKS, LINE, LINE), (LINKS * LINE) ** -0.5, 0.375, ((0, 8), (1, 4)))
    blocks_second = centred(key_list[13], (NX1, NY1, LINKS, LINE, LINE), (LINKS * LINE) ** -0.5, 0.375, ((0, 8), (1, 4)))
    blocks_third = centred(key_list[14], (NX2, NY2, LINKS, LINE, LINE), (LINKS * LINE) ** -0.5, 0.375, ((0, 8), (1, 4)))
    links_first = draw_links_first(jax.random.fold_in(key_list[18], 71), 0)
    links_second = draw_links_second(jax.random.fold_in(key_list[18], 71), 0)
    links_third = draw_links_third(jax.random.fold_in(key_list[18], 71), 0)
    return {"source_first": source_first, "source_second": source_second, "source_third": source_third, "source_fourth": source_fourth, "guess_first": guess_first, "guess_second": guess_second, "guess_third": guess_third, "guess_fourth": guess_fourth, "shift_first": shift_first, "shift_second": shift_second, "shift_third": shift_third, "shift_fourth": shift_fourth, "blocks_first": blocks_first, "blocks_second": blocks_second, "blocks_third": blocks_third, "links_first": links_first, "links_second": links_second, "links_third": links_third}


upper_edge = 14.0
lower_edge = upper_edge / 8.0


def operate(vector, diagonal):
    beside = jnp.roll(vector, 1, 0) + jnp.roll(vector, -1, 0)
    beside = beside + jnp.roll(vector, 1, 1) + jnp.roll(vector, -1, 1)
    beside = beside + jnp.roll(vector, 1, 3) + jnp.roll(vector, -1, 3)
    return (6.0 + diagonal[:, :, None, :]) * vector - beside


def chebyshev(source, initial, diagonal):
    centre = (upper_edge + lower_edge) / 2.0
    half_width = (upper_edge - lower_edge) / 2.0
    ratio_edge = centre / half_width
    factor = 1.0 / ratio_edge
    residual = source - operate(initial, diagonal)
    direction = residual / centre
    result = initial
    for sweep_index in range(DEGREE):
        result = result + direction
        if sweep_index + 1 < DEGREE:
            residual = residual - operate(direction, diagonal)
            factor_next = 1.0 / (2.0 * ratio_edge - factor)
            direction = factor_next * factor * direction + (2.0 * factor_next / half_width) * residual
            factor = factor_next
    return result


def prolong(coarse, link_ids, blocks):
    coarse_lines = coarse.astype(jnp.bfloat16).reshape((-1,) + coarse.shape[2:])

    def one_row(row_pair):
        row_links, row_blocks = row_pair
        picked = coarse_lines[row_links].astype(jnp.float32)
        return jnp.einsum("bkrj,bkij->bri", picked, row_blocks.astype(jnp.float32),
                          precision=lax.Precision.HIGHEST)

    return lax.map(one_row, (link_ids, blocks))


def reference(source_first, source_second, source_third, source_fourth,
              guess_first, guess_second, guess_third, guess_fourth,
              shift_first, shift_second, shift_third, shift_fourth,
              blocks_first, blocks_second, blocks_third,
              links_first, links_second, links_third):
    smooth_fourth = chebyshev(source_fourth, guess_fourth, shift_fourth)
    start_third = guess_third + prolong(smooth_fourth, links_third, blocks_third)
    smooth_third = chebyshev(source_third, start_third, shift_third)
    start_second = guess_second + prolong(smooth_third, links_second, blocks_second)
    smooth_second = chebyshev(source_second, start_second, shift_second)
    start_first = guess_first + prolong(smooth_second, links_first, blocks_first)
    smooth_first = chebyshev(source_first, start_first, shift_first)
    return (smooth_first, smooth_second, smooth_third, smooth_fourth)
```

```python
from functools import partial

import jax
import jax.numpy as jnp
from jax import lax
from jax.experimental import pallas as pl
from jax.experimental.pallas import tpu as pltpu
from jax.sharding import PartitionSpec as P

LEVELS = 4
REACH = 3
LAST = LEVELS - 1

upper_edge = 14.0
lower_edge = upper_edge / 8.0


def coefficients():
    centre = (upper_edge + lower_edge) / 2.0
    half_width = (upper_edge - lower_edge) / 2.0
    ratio = centre / half_width
    factor = 1.0 / ratio
    steps = []
    for _ in range(2):
        following = 1.0 / (2.0 * ratio - factor)
        steps.append((following * factor, 2.0 * following / half_width))
        factor = following
    (a1, b1), (a2, b2) = steps
    first = 1.0 / centre
    return {
        "own1": first * (a1 + b1 * centre),
        "side1": first * b1,
        "start2": first * (1.0 - a1 * b2 / b1),
        "own2": 1.0 + a2 + b2 / b1,
        "side2": b2,
    }


def beyond(index, length):
    return max(-index, index - length + 1, 0)


def plan(nx, ny, reach, box=False):
    def width(row):
        return reach if box else reach - beyond(row, nx)

    out = []
    far_x, far_y = -(-reach // nx), -(-reach // ny)
    for ox in range(-far_x, far_x + 1):
        for oy in range(-far_y, far_y + 1):
            if ox == 0 and oy == 0:
                continue
            runs = []
            for row in range(max(-ox * nx, -reach), min((1 - ox) * nx, nx + reach)):
                low = max(-oy * ny, -width(row))
                high = min((1 - oy) * ny, ny + width(row))
                if low >= high:
                    continue
                if runs and runs[-1][2:] == (low, high) and runs[-1][1] == row:
                    runs[-1] = (runs[-1][0], row + 1, low, high)
                else:
                    runs.append((row, row + 1, low, high))
            for top, end, low, high in runs:
                out.append(
                    (ox, oy, (top + ox * nx, low + oy * ny), (top, low), (end - top, high - low))
                )
    out.sort(key=lambda m: (-abs(m[0]), -abs(m[1]), m))
    return out


class Gather:
    def __init__(self, block, peers):
        self.block, self.peers = block, peers
        self.size = (block[0] * peers[0], block[1] * peers[1])
        self.u = self.around(3)
        self.s = self.around(2)
        self.slot = {cell: k for k, cell in enumerate(self.u)}

    def at(self, x, y):
        return x % self.size[0], y % self.size[1]

    def around(self, reach):
        nx, ny = self.block
        cells = []
        for x in range(-reach - 1, nx + reach + 1):
            for y in range(-reach - 1, ny + reach + 1):
                far = max(beyond(x, nx) - 1, 0) + max(beyond(y, ny) - 1, 0)
                if far <= reach and self.at(x, y) not in cells:
                    cells.append(self.at(x, y))
        return cells

    def messages(self):
        nx, ny = self.block

        def span(offset, count):
            return min(offset, count - offset)

        out = []
        for cell in self.u:
            ox, oy = cell[0] // nx, cell[1] // ny
            if ox or oy:
                own = self.slot[(cell[0] % nx, cell[1] % ny)]
                far = span(ox, self.peers[0]) + span(oy, self.peers[1])
                out.append((-far, -ox, -oy, own, self.slot[cell], cell in self.s))
        out.sort()
        return [m[1:] for m in out]


def modulo(value, size):
    if size & (size - 1) == 0:
        return jnp.bitwise_and(value, size - 1)
    return lax.rem(value, size)


def quotient(value, size):
    if size & (size - 1) == 0:
        return jnp.right_shift(value, size.bit_length() - 1)
    return lax.div(value, size)


class Counter:
    def __init__(self):
        self.used = 0

    def take(self):
        self.used += 1
        return self.used - 1


def message_count(dims, peers):
    total = 4 + sum(1 + 2 * m[-1] for m in Gather(dims[LAST], peers).messages())
    for level, (nx, ny) in enumerate(dims[:LAST]):
        total += len(plan(nx, ny, REACH)) + 2 * len(plan(nx, ny, REACH - 1))
        if level:
            total += len(plan(nx, ny, 1, True))
    return total


def partners(dims, peers):
    found = set()
    for nx, ny in dims[:LAST]:
        for m in plan(nx, ny, REACH) + plan(nx, ny, 1, True):
            found.add((m[0] % peers[0], m[1] % peers[1]))
            found.add((-m[0] % peers[0], -m[1] % peers[1]))
    for m in Gather(dims[LAST], peers).messages():
        found.add((m[0] % peers[0], m[1] % peers[1]))
        found.add((-m[0] % peers[0], -m[1] % peers[1]))
    return sorted(found)


def turned(shape):
    return shape[1] > shape[2]


def beside(centre, above, below):
    middle = centre[1:-1]
    line = middle.shape[-1]
    total = (centre[:-2] + centre[2:]) + (above + below)
    return total + (pltpu.roll(middle, 1, 3) + pltpu.roll(middle, line - 1, 3))


def smoothing(nx, ny, u, s, w0, w1, w2, q, p, finish):
    k = coefficients()

    def start(row):
        w = 2 - beyond(row, nx)
        count = ny + 2 * w
        near = beside(
            u[row + 3, pl.ds(2 - w, count + 2)],
            u[row + 2, pl.ds(3 - w, count)],
            u[row + 4, pl.ds(3 - w, count)],
        )
        own = u[row + 3, pl.ds(3 - w, count)]
        weight = w0[row + 2, pl.ds(2 - w, count)][:, None]
        q[row + 2, pl.ds(2 - w, count)] = (s[row + 2, pl.ds(2 - w, count)] - weight * own) + near

    def second(row):
        w = 1 - beyond(row, nx)
        count = ny + 2 * w
        near = beside(
            q[row + 2, pl.ds(1 - w, count + 2)],
            q[row + 1, pl.ds(2 - w, count)],
            q[row + 3, pl.ds(2 - w, count)],
        )
        own = q[row + 2, pl.ds(2 - w, count)]
        weight = w1[row + 1, pl.ds(1 - w, count)][:, None]
        p[row + 1, pl.ds(1 - w, count)] = weight * own + k["side1"] * near

    def third(row):
        near = beside(
            p[row + 1, pl.ds(0, ny + 2)], p[row, pl.ds(1, ny)], p[row + 2, pl.ds(1, ny)]
        )
        own = p[row + 1, pl.ds(1, ny)]
        begin = u[row + 3, pl.ds(3, ny)] + k["start2"] * q[row + 2, pl.ds(2, ny)]
        finish(row, (begin + w2[row][:, None] * own) + k["side2"] * near)

    for row in range(-2, nx + 6):
        if row < nx + 2:
            start(row)
        if -1 <= row - 2 < nx + 1:
            second(row - 2)
        if 0 <= row - 4 < nx:
            third(row - 4)


def upward(dims, peers, *refs):
    refs = list(refs)

    def take(count):
        got = refs[:count]
        del refs[:count]
        return got

    sources, guesses, shifts = take(4), take(4), take(4)
    blocks, link_inputs = take(3), take(3)
    start_out, source_out, w0_out, w1_out, w2_out = take(5)
    outs = [None] + take(3)
    U, S = [start_out] + take(2), [source_out] + take(2)
    D, H = take(3), take(4)
    W0, W1, W2 = [w0_out] + take(2), [w1_out] + take(2), [w2_out] + take(2)
    Q, PD = [None] + take(2), [None] + take(2)
    V, T, W = take(3)
    B, BT, C = take(3), take(3), take(3)
    K, DK, QK, PK = take(4)
    links = take(3)
    local_sem, send_sem, recv_sem = take(3)
    gz, gy = lax.axis_index("gz"), lax.axis_index("gy")
    k = coefficients()

    def at(ox, oy):
        return (lax.rem(gz + (ox % peers[0]), peers[0]), lax.rem(gy + (oy % peers[1]), peers[1]))

    barrier = pltpu.get_barrier_semaphore()
    company = partners(dims, peers)
    for ox, oy in company:
        pl.semaphore_signal(barrier, inc=1, device_id=at(ox, oy), device_id_type=pl.DeviceIdType.MESH)

    local = Counter()

    def fetch(source, target):
        copy = pltpu.make_async_copy(source, target, local_sem.at[local.take()])
        copy.start()
        return copy

    gather = Gather(dims[LAST], peers)
    last_x, last_y = dims[LAST]
    own_cells = [(x, y) for x in range(last_x) for y in range(last_y)]
    loads = [None] * LEVELS
    loads[LAST] = [fetch(shifts[LAST], H[LAST])]
    for x, y in own_cells:
        slot = gather.slot[(x, y)]
        loads[LAST].append(fetch(guesses[LAST].at[x, y], K.at[slot, 0]))
        loads[LAST].append(fetch(sources[LAST].at[x, y], K.at[slot, 1]))

    def own(ref, level, reach):
        nx, ny = dims[level]
        return ref.at[pl.ds(reach, nx), pl.ds(reach, ny)]

    for level in reversed(range(LAST)):
        loads[level] = [
            fetch(shifts[level], H[level]),
            fetch(sources[level], own(S[level], level, REACH - 1)),
            fetch(guesses[level], own(U[level], level, REACH)),
        ]
    for level in reversed(range(LAST)):
        loads[level].append(fetch(link_inputs[level], links[level]))
    block_loads = [None] * LAST
    for level in reversed(range(LAST)):
        block_loads[level] = fetch(blocks[level], B[level])

    for copy in loads[LAST]:
        copy.wait()
    for x, y in own_cells:
        DK[gather.slot[(x, y)]] = 6.0 + H[LAST][x, pl.ds(y, 1)]

    pl.semaphore_wait(barrier, len(company))

    counter = Counter()
    pending = []

    def send(source, target, device, later=True):
        index = counter.take()
        copy = pltpu.make_async_remote_copy(
            src_ref=source,
            dst_ref=target,
            send_sem=send_sem.at[index],
            recv_sem=recv_sem.at[index],
            device_id=device,
            device_id_type=pl.DeviceIdType.MESH,
        )
        copy.start()
        if later:
            pending.append(copy)
        return copy

    def rectangle(ref, corner, size, pad):
        return ref.at[pl.ds(corner[0] + pad, size[0]), pl.ds(corner[1] + pad, size[1])]

    def exchange(ref, pad, messages):
        return [
            send(rectangle(ref, source, size, pad), rectangle(ref, target, size, pad), at(ox, oy))
            for ox, oy, source, target, size in messages
        ]

    last = []
    for ox, oy, source, target, whole in gather.messages():
        if whole:
            last.append(send(K.at[source], K.at[target], at(ox, oy)))
            last.append(send(DK.at[source], DK.at[target], at(ox, oy)))
        else:
            last.append(send(K.at[source, 0], K.at[target, 0], at(ox, oy)))

    def diagonals(level):
        nx, ny = dims[level]
        for copy in loads[level]:
            copy.wait()
        for i in range(nx):
            for j in range(ny):
                D[level][i + 2, j + 2] = 6.0 + H[level][i, pl.ds(j, 1)]

    def sides(level, narrow=None):
        messages = plan(*dims[level], REACH - 1)
        copies = []
        for m in messages:
            ref = S[level] if narrow is None or m[0] == 0 else narrow
            copies += exchange(ref, 2, [m])
        return copies + exchange(D[level], 2, messages)

    def weigh(level):
        nx, ny = dims[level]
        for row in range(-2, nx + 2):
            w = 2 - beyond(row, nx)
            for col in range(-w, ny + w):
                d = jnp.broadcast_to(D[level][row + 2, col + 2], W0[level].shape[2:])
                W0[level][row + 2, col + 2] = d
                far = beyond(row, nx) + beyond(col, ny)
                if far <= 1:
                    W1[level][row + 1, col + 1] = k["own1"] - k["side1"] * d
                if far == 0:
                    W2[level][row, col] = k["own2"] - k["side2"] * d

    def turn(level):
        nx, ny = dims[level]
        block_loads[level].wait()
        line = B[level].shape[-1]

        def body(cell, carry):
            i, j = cell // ny, cell % ny
            for side in range(2):
                BT[level][i, j, pl.ds(side * line, line)] = B[level][i, j, side].T
            return carry

        lax.fori_loop(0, nx * ny, body, 0)

    def smooth(level):
        nx, ny = dims[level]

        def finish(row, result):
            outs[level][row] = result
            lines = result.reshape(result.shape[:1] + C[level - 1].shape[2:])
            C[level - 1][row + 1, pl.ds(1, ny)] = lines.astype(jnp.bfloat16)

        smoothing(
            nx, ny, U[level], S[level], W0[level], W1[level], W2[level], Q[level], PD[level], finish
        )

    def smooth_last():
        def near(ref, x, y):
            def cell(a, b):
                return ref[gather.slot[gather.at(a, b)]]

            middle = cell(x, y)
            total = (cell(x, y - 1) + cell(x, y + 1)) + (cell(x - 1, y) + cell(x + 1, y))
            line = middle.shape[-1]
            return middle, total + (pltpu.roll(middle, 1, 2) + pltpu.roll(middle, line - 1, 2))

        for x, y in gather.around(2):
            slot = gather.slot[(x, y)]
            middle, total = near(K.at[:, 0], x, y)
            QK[slot] = (K[slot, 1] - DK[slot] * middle) + total
        for x, y in gather.around(1):
            slot = gather.slot[(x, y)]
            middle, total = near(QK, x, y)
            PK[slot] = (k["own1"] - k["side1"] * DK[slot]) * middle + k["side1"] * total
        for x in range(-1, last_x + 1):
            for y in range(-1, last_y + 1):
                slot = gather.slot[gather.at(x, y)]
                middle, total = near(PK, x, y)
                begin = K[slot, 0] + k["start2"] * QK[slot]
                result = begin + (k["own2"] - k["side2"] * DK[slot]) * middle + k["side2"] * total
                if (x, y) in own_cells:
                    outs[LAST][x, y] = result
                C[LAST - 1][x + 1, y + 1] = result.reshape(C[LAST - 1].shape[2:]).astype(jnp.bfloat16)

    def prolong(level, rows):
        nx, ny = dims[level]
        cx, cy = dims[level + 1]
        full = (cx * peers[0], cy * peers[1])
        lift_x = full[0] + 1 - gz * cx
        lift_y = full[1] + 1 - gy * cy

        def pick(i, j, side):
            if turned((nx, ny, 2)):
                link = links[level][i, side, j]
            else:
                link = links[level][i, j, side]
            row = modulo(quotient(link, full[1]) + lift_x, full[0])
            col = modulo(modulo(link, full[1]) + lift_y, full[1])
            return C[level][jnp.minimum(row, cx + 1), jnp.minimum(col, cy + 1)]

        for i in rows:
            for j in range(ny):
                picked = jnp.concatenate([pick(i, j, 0), pick(i, j, 1)], axis=1)
                sums = lax.dot_general(
                    picked, BT[level][i, j], (((1,), (0,)), ((), ())), preferred_element_type=jnp.float32
                )
                u = U[level][i + REACH, j + REACH]
                u = u + sums.reshape(u.shape)
                U[level][i + REACH, j + REACH] = u
                if level == 0:
                    V[i + REACH, j + REACH] = u.reshape(sums.shape).astype(jnp.bfloat16)
                    if i == 0:
                        W[0, j] = sums.astype(jnp.bfloat16)
                    if i == nx - 1:
                        W[1, j] = sums.astype(jnp.bfloat16)

    def widen(source, target, pad, corner, size):
        for row in range(corner[0] + pad, corner[0] + pad + size[0]):
            cells = pl.ds(corner[1] + pad, size[1])
            value = source[row, cells].astype(jnp.float32)
            target[row, cells] = value.reshape(value.shape[:1] + target.shape[2:])

    diagonals(2)
    side2 = sides(2)
    diagonals(1)
    diagonals(0)
    nx, ny = dims[0]
    for i in range(nx):
        value = S[0][i + 2, pl.ds(2, ny)]
        T[i + 2, pl.ds(2, ny)] = value.reshape(value.shape[:1] + T.shape[2:]).astype(jnp.bfloat16)
    for level in reversed(range(LAST)):
        turn(level)

    def wait(copies):
        for copy in copies:
            copy.wait_recv()

    wait(last)
    smooth_last()
    prolong(2, range(dims[2][0]))
    begin2 = exchange(U[2], REACH, plan(*dims[2], REACH))
    side1 = sides(1)
    wait(side2)
    weigh(2)
    wait(begin2)
    smooth(2)
    coarse1 = exchange(C[1], 1, plan(*dims[2], 1, True))
    side0 = sides(0, T)
    wait(side1)
    weigh(1)
    wait(coarse1)
    prolong(1, range(dims[1][0]))
    begin1 = exchange(U[1], REACH, plan(*dims[1], REACH))
    messages = plan(*dims[0], REACH - 1)
    wait(side0)
    for m in messages:
        if m[0]:
            widen(T, S[0], 2, m[3], m[4])
    weigh(0)
    wait(begin1)
    smooth(1)
    coarse0 = exchange(C[0], 1, plan(*dims[1], 1, True))
    edges = ((1, nx - 1, -1, 1, 2), (-1, 0, nx, 0, 3))
    early = []
    for ox, row, place, _, _ in edges:
        cells = pl.ds(REACH, ny)
        source = U[0].at[row + REACH, cells]
        early.append(send(source, U[0].at[place + REACH, cells], at(ox, 0), False))
    wait(coarse0)
    for copy in early:
        copy.wait_send()

    messages = []
    for ox, oy, source, target, size in plan(*dims[0], REACH):
        if ox and not oy:
            shift = 1 if ox < 0 else 0
            source, target = (source[0] + shift, source[1]), (target[0] + shift, target[1])
            size = (size[0] - 1, size[1])
        messages.append((ox, oy, source, target, size))
    begin0 = []
    slim = []
    done = set()
    for rows in (range(min(REACH, nx)), range(max(nx - REACH, 0), nx), range(nx)):
        fresh = [i for i in rows if i not in done]
        done.update(fresh)
        prolong(0, fresh)
        for ox, row, place, slot, landing in edges:
            if row in fresh:
                slim.append((place, landing, send(W.at[slot], W.at[landing], at(ox, 0))))
        ready = [m for m in messages if all(m[2][0] + i in done for i in range(m[4][0]))]
        messages = [m for m in messages if m not in ready]
        for m in ready:
            begin0.append((m, exchange(V if m[0] else U[0], REACH, [m])[0]))
    wait(early)
    for place, landing, copy in slim:
        copy.wait_recv()
        value = W[landing].astype(jnp.float32)
        guess = U[0][place + REACH, pl.ds(REACH, ny)]
        U[0][place + REACH, pl.ds(REACH, ny)] = guess + value.reshape(guess.shape)
    for m, copy in begin0:
        copy.wait_recv()
        if m[0]:
            widen(V, U[0], REACH, m[3], m[4])
    for copy in pending:
        copy.wait_send()


def finishing(nx, ny, *refs):
    u, s, w0, w1, w2 = refs[:5]
    values, outs = refs[5:8], refs[8:12]
    q, p, o, sem = refs[12:]
    copies = []

    def store(source, target):
        copy = pltpu.make_async_copy(source, target, sem.at[len(copies)])
        copy.start()
        copies.append(copy)

    for value, out in zip(values, outs[1:]):
        store(value, out)

    def finish(row, result):
        o[row] = result
        store(o.at[row], outs[0].at[row])

    smoothing(nx, ny, u, s, w0, w1, w2, q, p, finish)
    for copy in copies:
        copy.wait()


def shards(peers, *args):
    dims = [x.shape[:2] for x in args[:4]]
    sides, width = args[0].shape[2:]
    tile = (8, width)
    line = (sides // 8,) + tile
    packed = (sides, width)
    args = [x.reshape(x.shape[:2] + line) for x in args[:8]] + list(args[8:])
    for n in range(15, 18):
        if turned(args[n].shape):
            args[n] = jnp.swapaxes(args[n], 1, 2)

    args = [pltpu.with_memory_space_constraint(x, pltpu.HBM) for x in args]

    def grown(level, extra, shape, dtype=jnp.float32):
        nx, ny = dims[level]
        return (nx + extra, ny + extra) + shape, dtype

    middle = (1, 2)
    results = [
        grown(0, 2 * REACH, line),
        grown(0, 4, line),
        grown(0, 4, tile),
        grown(0, 2, tile),
        grown(0, 0, tile),
    ] + [grown(level, 0, line) for level in (1, 2, 3)]
    slots = len(Gather(dims[LAST], peers).u)
    scratch = (
        [grown(n, 2 * REACH, line) for n in middle]
        + [grown(n, 4, line) for n in middle]
        + [grown(n, 4, (1, width)) for n in range(LAST)]
        + [grown(n, 0, (width,)) for n in range(LEVELS)]
        + [grown(n, 4, tile) for n in middle]
        + [grown(n, 2, tile) for n in middle]
        + [grown(n, 0, tile) for n in middle]
        + [grown(n, 4, line) for n in middle]
        + [grown(n, 2, line) for n in middle]
        + [grown(0, 2 * REACH, packed, jnp.bfloat16), grown(0, 4, packed, jnp.bfloat16)]
        + [((4, dims[0][1]) + packed, jnp.bfloat16)]
        + [(x.shape, x.dtype) for x in args[12:15]]
        + [(x.shape[:2] + (2 * width, width), x.dtype) for x in args[12:15]]
        + [grown(n, 2, packed, jnp.bfloat16) for n in range(1, LEVELS)]
        + [
            ((slots, 2) + line, jnp.float32),
            ((slots, 1, width), jnp.float32),
            ((slots,) + line, jnp.float32),
            ((slots,) + line, jnp.float32),
        ]
    )
    messages = message_count(dims, peers)
    anywhere = pl.BlockSpec(memory_space=pl.ANY)
    inside = pl.BlockSpec(memory_space=pltpu.VMEM)
    held = pl.pallas_call(
        partial(upward, dims, peers),
        out_shape=[pltpu.VMEM(*r) for r in results],
        in_specs=[anywhere] * 18,
        out_specs=[inside] * len(results),
        scratch_shapes=[pltpu.VMEM(*x) for x in scratch]
        + [pltpu.SMEM(x.shape, x.dtype) for x in args[15:]]
        + [
            pltpu.SemaphoreType.DMA((32,)),
            pltpu.SemaphoreType.DMA((messages,)),
            pltpu.SemaphoreType.DMA((messages,)),
        ],
        compiler_params=pltpu.CompilerParams(
            collective_id=0, has_side_effects=True, vmem_limit_bytes=40 * 2**20
        ),
    )(*args)
    nx, ny = dims[0]
    outs = pl.pallas_call(
        partial(finishing, nx, ny),
        out_shape=[jax.ShapeDtypeStruct(d + line, jnp.float32) for d in dims],
        in_specs=[inside] * len(results),
        out_specs=[anywhere] * LEVELS,
        scratch_shapes=[
            pltpu.VMEM(*grown(0, 4, line)),
            pltpu.VMEM(*grown(0, 2, line)),
            pltpu.VMEM(*grown(0, 0, line)),
            pltpu.SemaphoreType.DMA((nx + LEVELS,)),
        ],
        compiler_params=pltpu.CompilerParams(vmem_limit_bytes=16 * 2**20),
    )(*held)
    return tuple(x.reshape(x.shape[:2] + packed) for x in outs)


def solution(mesh):
    peers = (mesh.shape["gz"], mesh.shape["gy"])
    grid = P("gz", "gy")
    return jax.shard_map(
        partial(shards, peers),
        mesh=mesh,
        in_specs=(grid,) * 18,
        out_specs=(grid,) * 4,
        check_vma=False,
    )
```

```python
from functools import partial

import jax
import jax.numpy as jnp
from jax import lax
from jax.experimental import pallas as pl
from jax.experimental.pallas import tpu as pltpu
from jax.sharding import PartitionSpec as P

LEVELS = 4
REACH = 3
LAST = LEVELS - 1

upper_edge = 14.0
lower_edge = upper_edge / 8.0


def coefficients():
    centre = (upper_edge + lower_edge) / 2.0
    half_width = (upper_edge - lower_edge) / 2.0
    ratio = centre / half_width
    factor = 1.0 / ratio
    steps = []
    for _ in range(2):
        following = 1.0 / (2.0 * ratio - factor)
        steps.append((following * factor, 2.0 * following / half_width))
        factor = following
    (a1, b1), (a2, b2) = steps
    first = 1.0 / centre
    return {
        "own1": first * (a1 + b1 * centre),
        "side1": first * b1,
        "start2": first * (1.0 - a1 * b2 / b1),
        "own2": 1.0 + a2 + b2 / b1,
        "side2": b2,
    }


def beyond(index, length):
    return max(-index, index - length + 1, 0)


def plan(nx, ny, reach, box=False):
    def width(row):
        return reach if box else reach - beyond(row, nx)

    out = []
    far_x, far_y = -(-reach // nx), -(-reach // ny)
    for ox in range(-far_x, far_x + 1):
        for oy in range(-far_y, far_y + 1):
            if ox == 0 and oy == 0:
                continue
            runs = []
            for row in range(max(-ox * nx, -reach), min((1 - ox) * nx, nx + reach)):
                low = max(-oy * ny, -width(row))
                high = min((1 - oy) * ny, ny + width(row))
                if low >= high:
                    continue
                if runs and runs[-1][2:] == (low, high) and runs[-1][1] == row:
                    runs[-1] = (runs[-1][0], row + 1, low, high)
                else:
                    runs.append((row, row + 1, low, high))
            for top, end, low, high in runs:
                out.append(
                    (ox, oy, (top + ox * nx, low + oy * ny), (top, low), (end - top, high - low))
                )
    out.sort(key=lambda m: (-abs(m[0]), -abs(m[1]), m))
    return out


class Gather:
    def __init__(self, peers):
        self.size = peers
        rows = {x % peers[0]: abs(x) for x in (4, -4, 3, -3, 2, -2, 1, -1, 0)}
        self.far = {x: min(x, peers[0] - x) for x in rows}
        self.row = {x: k for k, x in enumerate(sorted(rows))}

    def around(self, reach):
        cells = []
        for x in range(-reach - 1, reach + 2):
            for y in range(-reach - 1, reach + 2):
                far = max(abs(x) - 1, 0) + max(abs(y) - 1, 0)
                cell = (x % self.size[0], y % self.size[1])
                if far <= reach and cell not in cells:
                    cells.append(cell)
        return cells

    def messages(self):
        out = []
        for x in self.row:
            for y in range(0, self.size[1], 2):
                if x or y:
                    out.append((-self.far[x] - min(y, self.size[1] - y), x, y, self.far[x] <= 3))
        out.sort()
        return [m[1:] for m in out]


def modulo(value, size):
    if size & (size - 1) == 0:
        return jnp.bitwise_and(value, size - 1)
    return lax.rem(value, size)


def quotient(value, size):
    if size & (size - 1) == 0:
        return jnp.right_shift(value, size.bit_length() - 1)
    return lax.div(value, size)


class Counter:
    def __init__(self):
        self.used = 0

    def take(self):
        self.used += 1
        return self.used - 1


def corners(nx, ny):
    out = []
    for ox in (1, -1):
        for far in range(1, REACH):
            target, source = (-far, nx - far) if ox > 0 else (nx - 1 + far, far - 1)
            out.append((ox, target, source, REACH - far))
    return out


def straight(nx, ny):
    near, rest = [], []
    for ox, oy, source, target, size in plan(nx, ny, REACH):
        if ox and oy:
            continue
        if not ox:
            rest.append((ox, oy, source, target, size))
            continue
        for row in range(size[0]):
            far = beyond(target[0] + row, nx)
            group = near if far < REACH else rest
            m = (ox, oy, (source[0] + row, source[1]), (target[0] + row, target[1]), (1, size[1]))
            group.append(m)
    near.sort(key=lambda m: beyond(m[3][0], nx))
    rest.sort(key=lambda m: -abs(m[0]))
    return near, rest


def message_count(dims, peers):
    total = 6 + 2 * sum(1 + m[-1] for m in Gather(peers).messages())
    for level, (nx, ny) in enumerate(dims[:LAST]):
        total += len(plan(nx, ny, REACH)) + 2 * len(plan(nx, ny, REACH - 1))
        if level:
            total += len(plan(nx, ny, 1, True)) + 4 * REACH
        else:
            total += 6 * REACH
    return total


def partners(dims, peers):
    found = set()
    for nx, ny in dims[:LAST]:
        for m in plan(nx, ny, REACH) + plan(nx, ny, 1, True):
            found.add((m[0] % peers[0], m[1] % peers[1]))
            found.add((-m[0] % peers[0], -m[1] % peers[1]))
    for x, y, _ in Gather(peers).messages():
        found.add((x, y))
        found.add((-x % peers[0], -y % peers[1]))
    return sorted(found)


def turned(shape):
    return shape[1] > shape[2]


def beside(centre, above, below):
    middle = centre[1:-1]
    line = middle.shape[-1]
    total = (centre[:-2] + centre[2:]) + (above + below)
    return total + (pltpu.roll(middle, 1, 3) + pltpu.roll(middle, line - 1, 3))


def smoothing(nx, ny, u, s, w0, w1, w2, q, p, finish, middle=None):
    k = coefficients()

    def wanted(row, margin):
        return middle is None or (margin <= row < nx - margin) == middle

    def start(row):
        w = 2 - beyond(row, nx)
        count = ny + 2 * w
        near = beside(
            u[row + 3, pl.ds(2 - w, count + 2)],
            u[row + 2, pl.ds(3 - w, count)],
            u[row + 4, pl.ds(3 - w, count)],
        )
        own = u[row + 3, pl.ds(3 - w, count)]
        weight = w0[row + 2, pl.ds(2 - w, count)][:, None]
        q(row)[row + 2, pl.ds(2 - w, count)] = (s[row + 2, pl.ds(2 - w, count)] - weight * own) + near

    def second(row):
        w = 1 - beyond(row, nx)
        count = ny + 2 * w
        near = beside(
            q(row)[row + 2, pl.ds(1 - w, count + 2)],
            q(row - 1)[row + 1, pl.ds(2 - w, count)],
            q(row + 1)[row + 3, pl.ds(2 - w, count)],
        )
        own = q(row)[row + 2, pl.ds(2 - w, count)]
        weight = w1[row + 1, pl.ds(1 - w, count)][:, None]
        p(row)[row + 1, pl.ds(1 - w, count)] = weight * own + k["side1"] * near

    def third(row):
        near = beside(
            p(row)[row + 1, pl.ds(0, ny + 2)],
            p(row - 1)[row, pl.ds(1, ny)],
            p(row + 1)[row + 2, pl.ds(1, ny)],
        )
        own = p(row)[row + 1, pl.ds(1, ny)]
        begin = u[row + 3, pl.ds(3, ny)] + k["start2"] * q(row)[row + 2, pl.ds(2, ny)]
        finish(row, (begin + w2[row][:, None] * own) + k["side2"] * near)

    for row in range(-2, nx + 6):
        if row < nx + 2 and wanted(row, 1):
            start(row)
        if -1 <= row - 2 < nx + 1 and wanted(row - 2, 2):
            second(row - 2)
        if 0 <= row - 4 < nx and wanted(row - 4, 3):
            third(row - 4)


def upward(dims, peers, *refs):
    refs = list(refs)

    def take(count):
        got = refs[:count]
        del refs[:count]
        return got

    sources, guesses, shifts = take(4), take(4), take(4)
    blocks, link_inputs = take(3), take(3)
    start_out, source_out, w0_out, w1_out, w2_out, q_out, p_out, middle_out = take(8)
    outs = [None] + take(3)
    U, S = [start_out] + take(2), [source_out] + take(2)
    D, H = take(3), take(4)
    W0, W1, W2 = [w0_out] + take(2), [w1_out] + take(2), [w2_out] + take(2)
    Q, PD = [q_out] + take(2), [p_out] + take(2)
    V, T, W, N = take(4)
    B, BT, C = take(3), take(3), take(3)
    K, DK, QK, PK = take(4)
    links = take(3)
    local_sem, send_sem, recv_sem = take(3)
    gz, gy = lax.axis_index("gz"), lax.axis_index("gy")
    k = coefficients()

    side = lax.rem(gy, 2)

    def at(ox, oy):
        oy = oy % peers[1] if isinstance(oy, int) else oy + peers[1]
        return (lax.rem(gz + (ox % peers[0]), peers[0]), lax.rem(gy + oy, peers[1]))

    partner = at(0, 1 - 2 * side)

    barrier = pltpu.get_barrier_semaphore()
    company = partners(dims, peers)
    for ox, oy in company:
        pl.semaphore_signal(barrier, inc=1, device_id=at(ox, oy), device_id_type=pl.DeviceIdType.MESH)

    local = Counter()

    def fetch(source, target):
        copy = pltpu.make_async_copy(source, target, local_sem.at[local.take()])
        copy.start()
        return copy

    gather = Gather(peers)
    loads = [None] * LEVELS
    loads[LAST] = [
        fetch(guesses[LAST].at[0, 0], K.at[gather.row[0], gy, 0]),
        fetch(sources[LAST].at[0, 0], K.at[gather.row[0], gy, 1]),
        fetch(shifts[LAST], H[LAST]),
    ]

    def own(ref, level, reach):
        nx, ny = dims[level]
        return ref.at[pl.ds(reach, nx), pl.ds(reach, ny)]

    for level in reversed(range(LAST)):
        loads[level] = [
            fetch(shifts[level], H[level]),
            fetch(sources[level], own(S[level], level, REACH - 1)),
            fetch(guesses[level], own(U[level], level, REACH)),
        ]
    for level in reversed(range(LAST)):
        loads[level].append(fetch(link_inputs[level], links[level]))
    block_loads = [None] * LAST
    for level in reversed(range(LAST)):
        block_loads[level] = fetch(blocks[level], B[level])

    for copy in loads[LAST]:
        copy.wait()
    DK[gather.row[0], gy] = 6.0 + H[LAST][0]

    pl.semaphore_wait(barrier, len(company))

    counter = Counter()
    pending = []

    def send(source, target, device, later=True):
        index = counter.take()
        copy = pltpu.make_async_remote_copy(
            src_ref=source,
            dst_ref=target,
            send_sem=send_sem.at[index],
            recv_sem=recv_sem.at[index],
            device_id=device,
            device_id_type=pl.DeviceIdType.MESH,
        )
        copy.start()
        if later:
            pending.append(copy)
        return copy

    def rectangle(ref, corner, size, pad):
        return ref.at[pl.ds(corner[0] + pad, size[0]), pl.ds(corner[1] + pad, size[1])]

    def exchange(ref, pad, messages):
        return [
            send(rectangle(ref, source, size, pad), rectangle(ref, target, size, pad), at(ox, oy))
            for ox, oy, source, target, size in messages
        ]

    def share(row, column, whole, device):
        cell = (row, column)
        if whole:
            return [
                send(K.at[cell], K.at[cell], device),
                send(DK.at[cell], DK.at[cell], device),
            ]
        return [send(K.at[cell].at[0], K.at[cell].at[0], device)]

    last = []
    for x, y, whole in gather.messages():
        source, target = (gather.row[0], gy), (gather.row[x], gy)
        copies = []
        if whole:
            copies.append(send(K.at[source], K.at[target], at(-x, -y)))
            copies.append(send(DK.at[source], DK.at[target], at(-x, -y)))
        else:
            copies.append(send(K.at[source].at[0], K.at[target].at[0], at(-x, -y)))
        last.append((gather.row[x], lax.rem(gy + y, peers[1]), whole, copies))
    handed = share(gather.row[0], gy, True, partner)

    def diagonals(level):
        nx, ny = dims[level]
        for copy in loads[level]:
            copy.wait()
        for i in range(nx):
            for j in range(ny):
                D[level][i + 2, j + 2] = 6.0 + H[level][i, pl.ds(j, 1)]

    def sides(level, narrow=None):
        messages = plan(*dims[level], REACH - 1)
        copies = []
        for m in messages:
            ref = S[level] if narrow is None or m[0] == 0 else narrow
            copies += exchange(ref, 2, [m])
        return copies + exchange(D[level], 2, messages)

    def weigh(level):
        nx, ny = dims[level]
        for row in range(-2, nx + 2):
            w = 2 - beyond(row, nx)
            for col in range(-w, ny + w):
                d = jnp.broadcast_to(D[level][row + 2, col + 2], W0[level].shape[2:])
                W0[level][row + 2, col + 2] = d
                far = beyond(row, nx) + beyond(col, ny)
                if far <= 1:
                    W1[level][row + 1, col + 1] = k["own1"] - k["side1"] * d
                if far == 0:
                    W2[level][row, col] = k["own2"] - k["side2"] * d

    def turn(level):
        nx, ny = dims[level]
        block_loads[level].wait()
        line = B[level].shape[-1]

        def body(i, carry):
            for j in range(ny):
                for part in range(2):
                    BT[level][i, j, pl.ds(part * line, line)] = B[level][i, j, part].T
            return carry

        lax.fori_loop(0, nx, body, 0)

    def relax(level, finish, middle=None):
        weights = W0[level], W1[level], W2[level]
        q, p = Q[level], PD[level]
        smoothing(*dims[level], U[level], S[level], *weights, lambda r: q, lambda r: p, finish, middle)

    def smooth(level):
        nx, ny = dims[level]

        def finish(row, result):
            outs[level][row] = result
            lines = result.reshape(result.shape[:1] + C[level - 1].shape[2:])
            C[level - 1][row + 1, pl.ds(1, ny)] = lines.astype(jnp.bfloat16)

        relax(level, finish)

    def smooth_last():
        column = [lax.rem(gy + y, peers[1]) for y in range(peers[1])]

        def place(x, y):
            return gather.row[x % peers[0]], column[y % peers[1]]

        def near(ref, x, y):
            middle = ref[place(x, y)]
            total = ref[place(x, y - 1)] + ref[place(x, y + 1)]
            total = total + (ref[place(x - 1, y)] + ref[place(x + 1, y)])
            line = middle.shape[-1]
            return middle, total + (pltpu.roll(middle, 1, 2) + pltpu.roll(middle, line - 1, 2))

        for x, y in gather.around(2):
            middle, total = near(K.at[:, :, 0], x, y)
            QK[place(x, y)] = (K[place(x, y) + (1,)] - DK[place(x, y)] * middle) + total
        for x, y in gather.around(1):
            middle, total = near(QK, x, y)
            weight = k["own1"] - k["side1"] * DK[place(x, y)]
            PK[place(x, y)] = weight * middle + k["side1"] * total
        for x in range(-1, 2):
            for y in range(-1, 2):
                middle, total = near(PK, x, y)
                weight = k["own2"] - k["side2"] * DK[place(x, y)]
                begin = K[place(x, y) + (0,)] + k["start2"] * QK[place(x, y)]
                result = begin + weight * middle + k["side2"] * total
                if x == 0 and y == 0:
                    outs[LAST][0, 0] = result
                C[LAST - 1][x + 1, y + 1] = result.reshape(C[LAST - 1].shape[2:]).astype(jnp.bfloat16)

    outer = []

    def begin(level):
        nx, ny = dims[level]
        u = U[level]
        near, rest = straight(nx, ny)
        first = list(zip(near, exchange(u, REACH, near)))
        later = []
        for ox, target, source, width in corners(nx, ny):
            start = side * (ny - width) + REACH
            stop = side * (-width - ny) + ny + REACH
            later.append(
                send(
                    u.at[source + REACH, pl.ds(start, width)],
                    u.at[target + REACH, pl.ds(stop, width)],
                    at(ox, 2 * side - 1),
                )
            )
        if level == 1:
            for slot, ox in enumerate((1, -1)):
                outer.append(send(N.at[slot], N.at[slot + 2], at(ox, 0)))
            rest = [m for m in rest if not m[0]]
        later += exchange(u, REACH, rest)
        return first, later

    def pass_on(level, first):
        nx, ny = dims[level]
        u = U[level]
        widths = {target: width for _, target, _, width in corners(nx, ny)}
        copies = []
        for m, copy in first:
            copy.wait_recv()
            row, width = m[3][0], widths[m[3][0]]
            start = (1 - side) * (ny - width) + REACH
            stop = (1 - side) * (-width - ny) + ny + REACH
            copies.append(
                send(
                    u.at[row + REACH, pl.ds(start, width)],
                    u.at[row + REACH, pl.ds(stop, width)],
                    partner,
                )
            )
        return copies

    def prolong(level, rows):
        nx, ny = dims[level]
        cx, cy = dims[level + 1]
        full = (cx * peers[0], cy * peers[1])
        lift_x = full[0] + 1 - gz * cx
        lift_y = full[1] + 1 - gy * cy

        def pick(i, j, side):
            if turned((nx, ny, 2)):
                link = links[level][i, side, j]
            else:
                link = links[level][i, j, side]
            row = modulo(quotient(link, full[1]) + lift_x, full[0])
            col = modulo(modulo(link, full[1]) + lift_y, full[1])
            return C[level][jnp.minimum(row, cx + 1), jnp.minimum(col, cy + 1)]

        for i in rows:
            for j in range(ny):
                picked = jnp.concatenate([pick(i, j, 0), pick(i, j, 1)], axis=1)
                sums = lax.dot_general(
                    picked, BT[level][i, j], (((1,), (0,)), ((), ())), preferred_element_type=jnp.float32
                )
                u = U[level][i + REACH, j + REACH]
                u = u + sums.reshape(u.shape)
                U[level][i + REACH, j + REACH] = u
                if level == 0:
                    V[i + REACH, j + REACH] = u.reshape(sums.shape).astype(jnp.bfloat16)
                    if i == 0:
                        W[0, j] = sums.astype(jnp.bfloat16)
                    if i == nx - 1:
                        W[1, j] = sums.astype(jnp.bfloat16)
                if level == 1:
                    for slot, row in enumerate((nx - REACH, REACH - 1)):
                        if i == row:
                            N[slot, j] = u.reshape(sums.shape).astype(jnp.bfloat16)

    def widen(source, target, pad, corner, size):
        for row in range(corner[0] + pad, corner[0] + pad + size[0]):
            cells = pl.ds(corner[1] + pad, size[1])
            value = source[row, cells].astype(jnp.float32)
            target[row, cells] = value.reshape(value.shape[:1] + target.shape[2:])

    diagonals(2)
    side2 = sides(2)
    diagonals(1)
    side1 = sides(1)
    diagonals(0)
    nx, ny = dims[0]
    for i in range(nx):
        value = S[0][i + 2, pl.ds(2, ny)]
        T[i + 2, pl.ds(2, ny)] = value.reshape(value.shape[:1] + T.shape[2:]).astype(jnp.bfloat16)
    for level in reversed(range(LAST)):
        turn(level)

    def wait(copies):
        for copy in copies:
            copy.wait_recv()

    for row, column, whole, copies in last:
        wait(copies)
        handed += share(row, column, whole, partner)
    wait(handed)
    smooth_last()
    prolong(2, range(dims[2][0]))
    first2, later2 = begin(2)
    wait(side2)
    weigh(2)
    handed2 = pass_on(2, first2)
    wait(later2 + handed2)
    smooth(2)
    coarse1 = exchange(C[1], 1, plan(*dims[2], 1, True))
    side0 = sides(0, T)
    wait(side1)
    weigh(1)
    wait(coarse1)
    prolong(1, range(dims[1][0]))
    first1, later1 = begin(1)
    messages = plan(*dims[0], REACH - 1)
    wait(side0)
    for m in messages:
        if m[0]:
            widen(T, S[0], 2, m[3], m[4])
    weigh(0)
    handed1 = pass_on(1, first1)
    for slot, copy in enumerate(outer):
        copy.wait_recv()
        row = (0, dims[1][0] + 2 * REACH - 1)[slot]
        value = N[slot + 2].astype(jnp.float32)
        cells = pl.ds(REACH, dims[1][1])
        U[1][row, cells] = value.reshape(value.shape[:1] + U[1].shape[2:])
    wait(later1 + handed1)
    smooth(1)
    coarse0 = exchange(C[0], 1, plan(*dims[1], 1, True))
    edges = ((1, nx - 1, -1, 1, 2), (-1, 0, nx, 0, 3))
    early = []
    for ox, row, place, _, _ in edges:
        cells = pl.ds(REACH, ny)
        source = U[0].at[row + REACH, cells]
        early.append(send(source, U[0].at[place + REACH, cells], at(ox, 0), False))
    wait(coarse0)
    for copy in early:
        copy.wait_send()

    third = range(min(REACH, nx)), range(max(nx - REACH, 0), nx), range(nx)
    segments = []
    for rows in third:
        segments.append([i for i in rows if not any(i in segment for segment in segments)])
    messages = []
    for ox, oy, source, target, size in plan(*dims[0], REACH):
        if ox and not oy:
            shift = 1 if ox < 0 else 0
            source, target = (source[0] + shift, source[1]), (target[0] + shift, target[1])
            messages.append((ox, oy, source, target, (size[0] - 1, size[1]), V))
        elif ox:
            messages.append((ox, oy, source, target, size, V))
        else:
            for segment in segments:
                for col in range(size[1]):
                    near = beyond(target[1] + col, ny) == 1
                    place = (segment[0], source[1] + col), (segment[0], target[1] + col)
                    messages.append((0, oy) + place + ((len(segment), 1), U[0] if near else V))
    sent = len(pending)
    begin0 = []
    slim = []
    done = set()
    for fresh in segments:
        done.update(fresh)
        prolong(0, fresh)
        for ox, row, place, slot, landing in edges:
            if row in fresh:
                slim.append((place, landing, send(W.at[slot], W.at[landing], at(ox, 0))))
        ready = [m for m in messages if all(m[2][0] + i in done for i in range(m[4][0]))]
        messages = [m for m in messages if m not in ready]
        for m in ready:
            begin0.append((m, exchange(m[5], REACH, [m[:5]])[0]))
    for copy in pending[:sent]:
        copy.wait_send()
    for m, copy in begin0:
        if not m[0]:
            copy.wait_recv()
            if m[5] is V:
                widen(V, U[0], REACH, m[3], m[4])

    def finish(row, result):
        middle_out[row] = result

    relax(0, finish, True)
    wait(early)
    for place, landing, copy in slim:
        copy.wait_recv()
        value = W[landing].astype(jnp.float32)
        guess = U[0][place + REACH, pl.ds(REACH, ny)]
        U[0][place + REACH, pl.ds(REACH, ny)] = guess + value.reshape(guess.shape)
    for m, copy in begin0:
        if m[0]:
            copy.wait_recv()
            widen(V, U[0], REACH, m[3], m[4])
    for copy in pending[sent:]:
        copy.wait_send()


def finishing(nx, ny, *refs):
    u, s, w0, w1, w2, q_held, p_held, middle = refs[:8]
    values, outs = refs[8:11], refs[11:15]
    q, p, o, sem = refs[15:]
    copies = []

    def store(source, target):
        copy = pltpu.make_async_copy(source, target, sem.at[len(copies)])
        copy.start()
        copies.append(copy)

    for value, out in zip(values, outs[1:]):
        store(value, out)
    for row in range(3, nx - 3):
        store(middle.at[row], outs[0].at[row])

    def finish(row, result):
        o[row] = result
        store(o.at[row], outs[0].at[row])

    def rows(held, fresh, margin):
        return lambda row: held if margin <= row < nx - margin else fresh

    smoothing(nx, ny, u, s, w0, w1, w2, rows(q_held, q, 1), rows(p_held, p, 2), finish, False)
    for copy in copies:
        copy.wait()


def shards(peers, *args):
    dims = [x.shape[:2] for x in args[:4]]
    sides, width = args[0].shape[2:]
    tile = (8, width)
    line = (sides // 8,) + tile
    packed = (sides, width)
    args = [x.reshape(x.shape[:2] + line) for x in args[:8]] + list(args[8:])
    for n in range(15, 18):
        if turned(args[n].shape):
            args[n] = jnp.swapaxes(args[n], 1, 2)

    args = [pltpu.with_memory_space_constraint(x, pltpu.HBM) for x in args]

    def grown(level, extra, shape, dtype=jnp.float32):
        nx, ny = dims[level]
        return (nx + extra, ny + extra) + shape, dtype

    middle = (1, 2)
    results = [
        grown(0, 2 * REACH, line),
        grown(0, 4, line),
        grown(0, 4, tile),
        grown(0, 2, tile),
        grown(0, 0, tile),
        grown(0, 4, line),
        grown(0, 2, line),
        grown(0, 0, line),
    ] + [grown(level, 0, line) for level in (1, 2, 3)]
    kept = (len(Gather(peers).row), peers[1])
    scratch = (
        [grown(n, 2 * REACH, line) for n in middle]
        + [grown(n, 4, line) for n in middle]
        + [grown(n, 4, (1, width)) for n in range(LAST)]
        + [grown(n, 0, (width,)) for n in range(LEVELS)]
        + [grown(n, 4, tile) for n in middle]
        + [grown(n, 2, tile) for n in middle]
        + [grown(n, 0, tile) for n in middle]
        + [grown(n, 4, line) for n in middle]
        + [grown(n, 2, line) for n in middle]
        + [grown(0, 2 * REACH, packed, jnp.bfloat16), grown(0, 4, packed, jnp.bfloat16)]
        + [((4, dims[n][1]) + packed, jnp.bfloat16) for n in (0, 1)]
        + [(x.shape, x.dtype) for x in args[12:15]]
        + [(x.shape[:2] + (2 * width, width), x.dtype) for x in args[12:15]]
        + [grown(n, 2, packed, jnp.bfloat16) for n in range(1, LEVELS)]
        + [
            (kept + (2,) + line, jnp.float32),
            (kept + (1, width), jnp.float32),
            (kept + line, jnp.float32),
            (kept + line, jnp.float32),
        ]
    )
    messages = message_count(dims, peers)
    anywhere = pl.BlockSpec(memory_space=pl.ANY)
    inside = pl.BlockSpec(memory_space=pltpu.VMEM)
    held = pl.pallas_call(
        partial(upward, dims, peers),
        out_shape=[pltpu.VMEM(*r) for r in results],
        in_specs=[anywhere] * 18,
        out_specs=[inside] * len(results),
        scratch_shapes=[pltpu.VMEM(*x) for x in scratch]
        + [pltpu.SMEM(x.shape, x.dtype) for x in args[15:]]
        + [
            pltpu.SemaphoreType.DMA((32,)),
            pltpu.SemaphoreType.DMA((messages,)),
            pltpu.SemaphoreType.DMA((messages,)),
        ],
        compiler_params=pltpu.CompilerParams(
            collective_id=0, has_side_effects=True, vmem_limit_bytes=40 * 2**20
        ),
    )(*args)
    nx, ny = dims[0]
    outs = pl.pallas_call(
        partial(finishing, nx, ny),
        out_shape=[jax.ShapeDtypeStruct(d + line, jnp.float32) for d in dims],
        in_specs=[inside] * len(results),
        out_specs=[anywhere] * LEVELS,
        scratch_shapes=[
            pltpu.VMEM(*grown(0, 4, line)),
            pltpu.VMEM(*grown(0, 2, line)),
            pltpu.VMEM(*grown(0, 0, line)),
            pltpu.SemaphoreType.DMA((nx + LEVELS,)),
        ],
        compiler_params=pltpu.CompilerParams(vmem_limit_bytes=16 * 2**20),
    )(*held)
    return tuple(x.reshape(x.shape[:2] + packed) for x in outs)


def solution(mesh):
    peers = (mesh.shape["gz"], mesh.shape["gy"])
    grid = P("gz", "gy")
    return jax.shard_map(
        partial(shards, peers),
        mesh=mesh,
        in_specs=(grid,) * 18,
        out_specs=(grid,) * 4,
        check_vma=False,
    )
```

```python
from functools import partial

import jax
import jax.numpy as jnp
from jax import lax
from jax.experimental import pallas as pl
from jax.experimental.pallas import tpu as pltpu
from jax.sharding import PartitionSpec as P

LEVELS = 4
REACH = 3
LAST = LEVELS - 1

upper_edge = 14.0
lower_edge = upper_edge / 8.0


def coefficients():
    centre = (upper_edge + lower_edge) / 2.0
    half_width = (upper_edge - lower_edge) / 2.0
    ratio = centre / half_width
    factor = 1.0 / ratio
    steps = []
    for _ in range(2):
        following = 1.0 / (2.0 * ratio - factor)
        steps.append((following * factor, 2.0 * following / half_width))
        factor = following
    (a1, b1), (a2, b2) = steps
    first = 1.0 / centre
    return {
        "own1": first * (a1 + b1 * centre),
        "side1": first * b1,
        "start2": first * (1.0 - a1 * b2 / b1),
        "own2": 1.0 + a2 + b2 / b1,
        "side2": b2,
    }


def beyond(index, length):
    return max(-index, index - length + 1, 0)


def plan(nx, ny, reach, box=False):
    def width(row):
        return reach if box else reach - beyond(row, nx)

    out = []
    far_x, far_y = -(-reach // nx), -(-reach // ny)
    for ox in range(-far_x, far_x + 1):
        for oy in range(-far_y, far_y + 1):
            if ox == 0 and oy == 0:
                continue
            runs = []
            for row in range(max(-ox * nx, -reach), min((1 - ox) * nx, nx + reach)):
                low = max(-oy * ny, -width(row))
                high = min((1 - oy) * ny, ny + width(row))
                if low >= high:
                    continue
                if runs and runs[-1][2:] == (low, high) and runs[-1][1] == row:
                    runs[-1] = (runs[-1][0], row + 1, low, high)
                else:
                    runs.append((row, row + 1, low, high))
            for top, end, low, high in runs:
                out.append(
                    (ox, oy, (top + ox * nx, low + oy * ny), (top, low), (end - top, high - low))
                )
    out.sort(key=lambda m: (-abs(m[0]), -abs(m[1]), m))
    return out


class Gather:
    def __init__(self, peers):
        self.size = peers
        rows = {x % peers[0]: abs(x) for x in (4, -4, 3, -3, 2, -2, 1, -1, 0)}
        self.far = {x: min(x, peers[0] - x) for x in rows}
        self.row = {x: k for k, x in enumerate(sorted(rows))}

    def around(self, reach):
        cells = []
        for x in range(-reach - 1, reach + 2):
            for y in range(-reach - 1, reach + 2):
                far = max(abs(x) - 1, 0) + max(abs(y) - 1, 0)
                cell = (x % self.size[0], y % self.size[1])
                if far <= reach and cell not in cells:
                    cells.append(cell)
        return cells

    def messages(self):
        out = []
        for x in self.row:
            for y in range(0, self.size[1], 2):
                if x or y:
                    out.append((-self.far[x] - min(y, self.size[1] - y), x, y, self.far[x] <= 3))
        out.sort()
        return [m[1:] for m in out]


def modulo(value, size):
    if size & (size - 1) == 0:
        return jnp.bitwise_and(value, size - 1)
    return lax.rem(value, size)


def quotient(value, size):
    if size & (size - 1) == 0:
        return jnp.right_shift(value, size.bit_length() - 1)
    return lax.div(value, size)


class Counter:
    def __init__(self):
        self.used = 0

    def take(self):
        self.used += 1
        return self.used - 1


def corners(nx, ny):
    out = []
    for ox in (1, -1):
        for far in range(1, REACH):
            target, source = (-far, nx - far) if ox > 0 else (nx - 1 + far, far - 1)
            out.append((ox, target, source, REACH - far))
    return out


def straight(nx, ny):
    near, rest = [], []
    for ox, oy, source, target, size in plan(nx, ny, REACH):
        if ox and oy:
            continue
        if not ox:
            rest.append((ox, oy, source, target, size))
            continue
        for row in range(size[0]):
            far = beyond(target[0] + row, nx)
            group = near if far < REACH else rest
            m = (ox, oy, (source[0] + row, source[1]), (target[0] + row, target[1]), (1, size[1]))
            group.append(m)
    near.sort(key=lambda m: beyond(m[3][0], nx))
    rest.sort(key=lambda m: -abs(m[0]))
    return near, rest


def slab(nx, reach, peers):
    far = -(-reach // nx)
    out = []
    for ox in range(-far, far + 1):
        for oy in range(0, peers[1], 2):
            top, end = max(-ox * nx, -reach), min((1 - ox) * nx, nx + reach)
            if (ox or oy) and top < end:
                out.append((ox, oy, top + ox * nx, top, end - top))
    out.sort(key=lambda m: (abs(m[0]) + min(m[1], peers[1] - m[1]), m))
    return out


def message_count(dims, peers):
    total = 14 + 2 * sum(1 + m[-1] for m in Gather(peers).messages())
    third = dims[LAST - 1][0]
    total += 2 * (1 + len(slab(third, REACH + 1, peers)) + 2 * len(slab(third, REACH, peers)) + 2)
    for level, (nx, ny) in enumerate(dims[: LAST - 1]):
        total += len(plan(nx, ny, REACH)) + 2 * len(plan(nx, ny, REACH - 1))
        if level:
            total += len(plan(nx, ny, 1, True)) + 4 * REACH
        else:
            total += 6 * REACH
    return total


def partners(dims, peers):
    found = set()
    for nx, ny in dims[: LAST - 1]:
        for m in plan(nx, ny, REACH) + plan(nx, ny, 1, True):
            found.add((m[0] % peers[0], m[1] % peers[1]))
            found.add((-m[0] % peers[0], -m[1] % peers[1]))
    around = [m[:2] for m in slab(dims[LAST - 1][0], REACH + 1, peers)]
    for x, y in around + [m[:2] for m in Gather(peers).messages()]:
        found.add((x % peers[0], y % peers[1]))
        found.add((-x % peers[0], -y % peers[1]))
    return sorted(found)


def turned(shape):
    return shape[1] > shape[2]


def beside(centre, above, below):
    middle = centre[1:-1]
    line = middle.shape[-1]
    total = centre[:-2] + centre[2:]
    for other in (above, below):
        if other is not None:
            total = total + other
    return total + (pltpu.roll(middle, 1, 3) + pltpu.roll(middle, line - 1, 3))


def smoothing(nx, ny, u, s, w0, w1, w2, q, p, finish, middle=None, held=None):
    k = coefficients()

    def share(row, margin):
        if middle is None:
            return "all"
        inside = margin <= row < nx - margin
        edge = row in (margin - 1, nx - margin) and nx > 2 * REACH
        if middle:
            return "all" if inside else "inner" if edge else None
        return None if inside else "outer" if edge else "all"

    def around(ref, row, pad, cells, part, margin):
        sides = []
        for other in (row - 1, row + 1):
            outer = (other < row) == (row == margin - 1)
            wanted = part == "all" or (part == "outer") == outer
            sides.append(ref(other)[other + pad, cells] if wanted else None)
        return [x for x in sides if x is not None][0] if part == "outer" else sides

    def start(row, part):
        w = 2 - beyond(row, nx)
        count = ny + 2 * w
        cells, inner = pl.ds(2 - w, count), pl.ds(3 - w, count)
        others = around(lambda _: u, row, 3, inner, part, 1)
        if part == "outer":
            q(row)[row + 2, cells] = held[0][row + 2, cells] + others
            return
        near = beside(u[row + 3, pl.ds(2 - w, count + 2)], *others)
        weight = w0[row + 2, cells][:, None]
        q(row)[row + 2, cells] = (s[row + 2, cells] - weight * u[row + 3, inner]) + near

    def second(row, part):
        w = 1 - beyond(row, nx)
        count = ny + 2 * w
        cells, inner = pl.ds(1 - w, count), pl.ds(2 - w, count)
        others = around(q, row, 2, inner, part, 2)
        if part == "outer":
            p(row)[row + 1, cells] = held[1][row + 1, cells] + k["side1"] * others
            return
        near = beside(q(row)[row + 2, pl.ds(1 - w, count + 2)], *others)
        weight = w1[row + 1, cells][:, None]
        p(row)[row + 1, cells] = weight * q(row)[row + 2, inner] + k["side1"] * near

    def third(row, part):
        cells = pl.ds(1, ny)
        others = around(p, row, 1, cells, part, 3)
        if part == "outer":
            finish(row, held[2][row] + k["side2"] * others)
            return
        near = beside(p(row)[row + 1, pl.ds(0, ny + 2)], *others)
        begin = u[row + 3, pl.ds(3, ny)] + k["start2"] * q(row)[row + 2, pl.ds(2, ny)]
        finish(row, (begin + w2[row][:, None] * p(row)[row + 1, cells]) + k["side2"] * near)

    for row in range(-2, nx + 6):
        if row < nx + 2 and share(row, 1):
            start(row, share(row, 1))
        if -1 <= row - 2 < nx + 1 and share(row - 2, 2):
            second(row - 2, share(row - 2, 2))
        if 0 <= row - 4 < nx and share(row - 4, 3):
            third(row - 4, share(row - 4, 3))


def upward(dims, peers, *refs):
    refs = list(refs)

    def take(count):
        got = refs[:count]
        del refs[:count]
        return got

    sources, guesses, shifts = take(4), take(4), take(4)
    blocks, link_inputs = take(3), take(3)
    start_out, source_out, w0_out, w1_out, w2_out, q_out, p_out, middle_out = take(8)
    outs = [None] + take(3)
    U, S = [start_out] + take(2), [source_out] + take(2)
    D, H = take(3), take(4)
    W0, W1, W2 = [w0_out] + take(2), [w1_out] + take(2), [w2_out] + take(2)
    Q, PD = [q_out] + take(2), [p_out] + take(2)
    V, T, W, N, M = take(5)
    B, BT, C = take(3), take(3), take(3)
    K, DK, QK, PK = take(4)
    R = refs.pop(0)
    links = take(3)
    local_sem, send_sem, recv_sem = take(3)
    gz, gy = lax.axis_index("gz"), lax.axis_index("gy")
    k = coefficients()

    side = lax.rem(gy, 2)

    def at(ox, oy):
        oy = oy % peers[1] if isinstance(oy, int) else oy + peers[1]
        return (lax.rem(gz + (ox % peers[0]), peers[0]), lax.rem(gy + oy, peers[1]))

    partner = at(0, 1 - 2 * side)

    barrier = pltpu.get_barrier_semaphore()
    company = partners(dims, peers)
    for ox, oy in company:
        pl.semaphore_signal(barrier, inc=1, device_id=at(ox, oy), device_id_type=pl.DeviceIdType.MESH)

    local = Counter()

    def fetch(source, target):
        copy = pltpu.make_async_copy(source, target, local_sem.at[local.take()])
        copy.start()
        return copy

    gather = Gather(peers)
    loads = [None] * LEVELS
    loads[LAST] = [
        fetch(guesses[LAST].at[0, 0], K.at[gather.row[0], gy, 0]),
        fetch(sources[LAST].at[0, 0], K.at[gather.row[0], gy, 1]),
        fetch(shifts[LAST], H[LAST]),
    ]

    def own(ref, level, reach):
        nx, ny = dims[level]
        return ref.at[pl.ds(reach, nx), pl.ds(reach, ny)]

    third = LAST - 1
    mine = pl.ds(gy * dims[third][1], dims[third][1])
    for level in reversed(range(LAST)):
        loads[level] = [fetch(shifts[level], H[level])]
        if level == third:
            rows = dims[third][0]
            loads[level].append(fetch(sources[level], S[level].at[pl.ds(REACH, rows), mine]))
            loads[level].append(fetch(guesses[level], U[level].at[pl.ds(REACH + 1, rows), mine]))
        else:
            loads[level].append(fetch(sources[level], own(S[level], level, REACH - 1)))
            loads[level].append(fetch(guesses[level], own(U[level], level, REACH)))
    for level in reversed(range(LAST)):
        loads[level].append(fetch(link_inputs[level], links[level]))
    block_loads = [None] * LAST
    for level in reversed(range(LAST)):
        block_loads[level] = fetch(blocks[level], B[level])

    for copy in loads[LAST]:
        copy.wait()
    DK[gather.row[0], gy] = 6.0 + H[LAST][0]

    pl.semaphore_wait(barrier, len(company))

    counter = Counter()
    pending = []

    def send(source, target, device, later=True):
        index = counter.take()
        copy = pltpu.make_async_remote_copy(
            src_ref=source,
            dst_ref=target,
            send_sem=send_sem.at[index],
            recv_sem=recv_sem.at[index],
            device_id=device,
            device_id_type=pl.DeviceIdType.MESH,
        )
        copy.start()
        if later:
            pending.append(copy)
        return copy

    def rectangle(ref, corner, size, pad):
        return ref.at[pl.ds(corner[0] + pad, size[0]), pl.ds(corner[1] + pad, size[1])]

    def exchange(ref, pad, messages):
        return [
            send(rectangle(ref, source, size, pad), rectangle(ref, target, size, pad), at(ox, oy))
            for ox, oy, source, target, size in messages
        ]

    def share(row, column, whole, device):
        cell = (row, column)
        if whole:
            return [
                send(K.at[cell], K.at[cell], device),
                send(DK.at[cell], DK.at[cell], device),
            ]
        return [send(K.at[cell].at[0], K.at[cell].at[0], device)]

    last = []
    for x, y, whole in gather.messages():
        source, target = (gather.row[0], gy), (gather.row[x], gy)
        copies = []
        if whole:
            copies.append(send(K.at[source], K.at[target], at(-x, -y)))
            copies.append(send(DK.at[source], DK.at[target], at(-x, -y)))
        else:
            copies.append(send(K.at[source].at[0], K.at[target].at[0], at(-x, -y)))
        last.append((gather.row[x], lax.rem(gy + y, peers[1]), whole, copies))
    handed = share(gather.row[0], gy, True, partner)

    def diagonals(level):
        nx, ny = dims[level]
        for copy in loads[level]:
            copy.wait()
        for i in range(nx):
            for j in range(ny):
                d = 6.0 + H[level][i, pl.ds(j, 1)]
                if level == third:
                    D[level][i + REACH, gy * ny + j] = d
                else:
                    D[level][i + 2, j + 2] = d

    def sides(level, narrow=None):
        messages = plan(*dims[level], REACH - 1)
        copies = []
        for m in messages:
            ref = S[level] if narrow is None or m[0] == 0 else narrow
            copies += exchange(ref, 2, [m])
        return copies + exchange(D[level], 2, messages)

    def sides_second():
        nx, ny = dims[1]
        s = S[1]
        copies, near, thin = [], [], []
        for slot, row in enumerate((nx - 2, 1)):
            value = s[row + 2, pl.ds(2, ny)]
            M[slot] = value.reshape(value.shape[:1] + M.shape[2:]).astype(jnp.bfloat16)
        for slot, (ox, source, target) in enumerate(((1, nx - 1, -1), (-1, 0, nx))):
            cells = pl.ds(2, ny)
            near.append((target, send(s.at[source + 2, cells], s.at[target + 2, cells], at(ox, 0))))
            start, stop = side * (ny - 1) + 2, side * (-1 - ny) + ny + 2
            corner = s.at[source + 2, pl.ds(start, 1)], s.at[target + 2, pl.ds(stop, 1)]
            copies.append(send(*corner, at(ox, 2 * side - 1)))
            thin.append(send(M.at[slot], M.at[slot + 2], at(ox, 0)))
        messages = plan(nx, ny, REACH - 1)
        copies += exchange(s, 2, [m for m in messages if not m[0]])
        return copies + exchange(D[1], 2, messages), near, thin

    def finish_second(copies, near, thin):
        nx, ny = dims[1]
        s = S[1]
        handed = []
        for target, copy in near:
            copy.wait_recv()
            start = (1 - side) * (ny - 1) + 2
            stop = (1 - side) * (-1 - ny) + ny + 2
            corner = s.at[target + 2, pl.ds(start, 1)], s.at[target + 2, pl.ds(stop, 1)]
            handed.append(send(*corner, partner))
        for slot, copy in enumerate(thin):
            copy.wait_recv()
            value = M[slot + 2].astype(jnp.float32)
            row = (0, nx + 3)[slot]
            s[row, pl.ds(2, ny)] = value.reshape(value.shape[:1] + s.shape[2:])
        wait(copies + handed)

    def weigh(level):
        nx, ny = dims[level]
        for row in range(-2, nx + 2):
            w = 2 - beyond(row, nx)
            for col in range(-w, ny + w):
                d = jnp.broadcast_to(D[level][row + 2, col + 2], W0[level].shape[2:])
                W0[level][row + 2, col + 2] = d
                far = beyond(row, nx) + beyond(col, ny)
                if far <= 1:
                    W1[level][row + 1, col + 1] = k["own1"] - k["side1"] * d
                if far == 0:
                    W2[level][row, col] = k["own2"] - k["side2"] * d

    def spread(ref, reach):
        nx = dims[third][0]
        whole = pl.ds(reach, nx)
        copies = []
        for ox, oy, source, target, count in slab(nx, REACH + 1 if ref is U[third] else REACH, peers):
            start, stop = pl.ds(source + reach, count), pl.ds(target + reach, count)
            column = lax.rem(gy + peers[1] - oy, peers[1]) * dims[third][1]
            copy = send(ref.at[start, mine], ref.at[stop, mine], at(ox, oy))
            copies.append((stop, pl.ds(column, dims[third][1]), copy))
        return copies, [send(ref.at[whole, mine], ref.at[whole, mine], partner)]

    def hand(ref, copies, handed):
        for rows, columns, copy in copies:
            copy.wait_recv()
            handed.append(send(ref.at[rows, columns], ref.at[rows, columns], partner))

    def weigh_third():
        nx, columns = dims[third][0], D[third].shape[1]
        for row in range(-REACH, nx + REACH):
            for col in range(columns):
                d = jnp.broadcast_to(D[third][row + REACH, col], W0[third].shape[2:])
                W0[third][row + REACH, col] = d
                if -2 <= row < nx + 2:
                    W1[third][row + 2, col] = k["own1"] - k["side1"] * d
                if -1 <= row < nx + 1:
                    W2[third][row + 1, col] = k["own2"] - k["side2"] * d

    def smooth_third():
        nx, ny = dims[third]
        u, s, q, p = U[third], S[third], Q[third], PD[third]

        def near(ref, row):
            middle = ref[row]
            ring = jnp.concatenate([middle[-1:], middle, middle[:1]], axis=0)
            return middle, beside(ring, ref[row - 1], ref[row + 1])

        for row in range(-3, nx + 3):
            middle, total = near(u, row + 4)
            q[row + 3] = (s[row + 3] - W0[third][row + 3][:, None] * middle) + total
        for row in range(-2, nx + 2):
            middle, total = near(q, row + 3)
            p[row + 2] = W1[third][row + 2][:, None] * middle + k["side1"] * total
        for row in range(-1, nx + 1):
            middle, total = near(p, row + 2)
            begin = u[row + 4] + k["start2"] * q[row + 3]
            result = begin + W2[third][row + 1][:, None] * middle + k["side2"] * total
            lines = result.reshape(result.shape[:1] + C[third - 1].shape[2:])
            C[third - 1][row + 1] = lines.astype(jnp.bfloat16)
            if 0 <= row < nx:
                R[row] = result
        for row in range(nx):
            outs[third][row] = R[row, mine]

    def turn(level):
        nx, ny = dims[level]
        block_loads[level].wait()
        line = B[level].shape[-1]

        def body(i, carry):
            for j in range(ny):
                for part in range(2):
                    BT[level][i, j, pl.ds(part * line, line)] = B[level][i, j, part].T
            return carry

        lax.fori_loop(0, nx, body, 0)

    def relax(level, finish, middle=None):
        weights = W0[level], W1[level], W2[level]
        q, p = Q[level], PD[level]
        smoothing(*dims[level], U[level], S[level], *weights, lambda r: q, lambda r: p, finish, middle)

    def smooth(level):
        nx, ny = dims[level]

        def finish(row, result):
            outs[level][row] = result
            lines = result.reshape(result.shape[:1] + C[level - 1].shape[2:])
            C[level - 1][row + 1, pl.ds(1, ny)] = lines.astype(jnp.bfloat16)

        relax(level, finish)

    def smooth_last():
        column = [lax.rem(gy + y, peers[1]) for y in range(peers[1])]

        def place(x, y):
            return gather.row[x % peers[0]], column[y % peers[1]]

        def near(ref, x, y):
            middle = ref[place(x, y)]
            total = ref[place(x, y - 1)] + ref[place(x, y + 1)]
            total = total + (ref[place(x - 1, y)] + ref[place(x + 1, y)])
            line = middle.shape[-1]
            return middle, total + (pltpu.roll(middle, 1, 2) + pltpu.roll(middle, line - 1, 2))

        for x, y in gather.around(2):
            middle, total = near(K.at[:, :, 0], x, y)
            QK[place(x, y)] = (K[place(x, y) + (1,)] - DK[place(x, y)] * middle) + total
        for x, y in gather.around(1):
            middle, total = near(QK, x, y)
            weight = k["own1"] - k["side1"] * DK[place(x, y)]
            PK[place(x, y)] = weight * middle + k["side1"] * total
        for x in range(-1, 2):
            for y in range(-1, 2):
                middle, total = near(PK, x, y)
                weight = k["own2"] - k["side2"] * DK[place(x, y)]
                begin = K[place(x, y) + (0,)] + k["start2"] * QK[place(x, y)]
                result = begin + weight * middle + k["side2"] * total
                if x == 0 and y == 0:
                    outs[LAST][0, 0] = result
                C[LAST - 1][x + 1, y + 1] = result.reshape(C[LAST - 1].shape[2:]).astype(jnp.bfloat16)

    outer = []

    def begin(level):
        nx, ny = dims[level]
        u = U[level]
        near, rest = straight(nx, ny)
        first = list(zip(near, exchange(u, REACH, near)))
        later = []
        for ox, target, source, width in corners(nx, ny):
            start = side * (ny - width) + REACH
            stop = side * (-width - ny) + ny + REACH
            later.append(
                send(
                    u.at[source + REACH, pl.ds(start, width)],
                    u.at[target + REACH, pl.ds(stop, width)],
                    at(ox, 2 * side - 1),
                )
            )
        if level == 1:
            for slot, ox in enumerate((1, -1)):
                outer.append(send(N.at[slot], N.at[slot + 2], at(ox, 0)))
            rest = [m for m in rest if not m[0]]
        later += exchange(u, REACH, rest)
        return first, later

    def pass_on(level, first):
        nx, ny = dims[level]
        u = U[level]
        widths = {target: width for _, target, _, width in corners(nx, ny)}
        copies = []
        for m, copy in first:
            copy.wait_recv()
            row, width = m[3][0], widths[m[3][0]]
            start = (1 - side) * (ny - width) + REACH
            stop = (1 - side) * (-width - ny) + ny + REACH
            copies.append(
                send(
                    u.at[row + REACH, pl.ds(start, width)],
                    u.at[row + REACH, pl.ds(stop, width)],
                    partner,
                )
            )
        return copies

    def prolong(level, rows):
        nx, ny = dims[level]
        cx, cy = dims[level + 1]
        full = (cx * peers[0], cy * peers[1])
        lift_x = full[0] + 1 - gz * cx
        lift_y = full[1] + 1 - gy * cy

        def pick(i, j, side):
            if turned((nx, ny, 2)):
                link = links[level][i, side, j]
            else:
                link = links[level][i, j, side]
            row = modulo(quotient(link, full[1]) + lift_x, full[0])
            col = modulo(link, full[1])
            if level + 1 != third:
                col = jnp.minimum(modulo(col + lift_y, full[1]), cy + 1)
            return C[level][jnp.minimum(row, cx + 1), col]

        for i in rows:
            for j in range(ny):
                picked = jnp.concatenate([pick(i, j, 0), pick(i, j, 1)], axis=1)
                sums = lax.dot_general(
                    picked, BT[level][i, j], (((1,), (0,)), ((), ())), preferred_element_type=jnp.float32
                )
                place = i + REACH, j + REACH
                if level == third:
                    place = i + REACH + 1, gy * ny + j
                u = U[level][place]
                u = u + sums.reshape(u.shape)
                U[level][place] = u
                if level == 0:
                    V[i + REACH, j + REACH] = u.reshape(sums.shape).astype(jnp.bfloat16)
                    if i == 0:
                        W[0, j] = sums.astype(jnp.bfloat16)
                    if i == nx - 1:
                        W[1, j] = sums.astype(jnp.bfloat16)
                if level == 1:
                    for slot, row in enumerate((nx - REACH, REACH - 1)):
                        if i == row:
                            N[slot, j] = u.reshape(sums.shape).astype(jnp.bfloat16)

    def widen(source, target, pad, corner, size):
        for row in range(corner[0] + pad, corner[0] + pad + size[0]):
            cells = pl.ds(corner[1] + pad, size[1])
            value = source[row, cells].astype(jnp.float32)
            target[row, cells] = value.reshape(value.shape[:1] + target.shape[2:])

    diagonals(2)
    side2 = spread(S[third], REACH), spread(D[third], REACH)
    diagonals(1)
    diagonals(0)
    nx, ny = dims[0]
    for i in range(nx):
        value = S[0][i + 2, pl.ds(2, ny)]
        T[i + 2, pl.ds(2, ny)] = value.reshape(value.shape[:1] + T.shape[2:]).astype(jnp.bfloat16)
    for level in reversed(range(LAST)):
        turn(level)

    def wait(copies):
        for copy in copies:
            copy.wait_recv()

    for row, column, whole, copies in last:
        wait(copies)
        handed += share(row, column, whole, partner)
    wait(handed)
    smooth_last()
    prolong(2, range(dims[2][0]))
    first2, later2 = spread(U[third], REACH + 1)
    side1 = sides_second()
    side0 = sides(0, T)
    for ref, (copies, handed) in zip((S[third], D[third]), side2):
        hand(ref, copies, handed)
    hand(U[third], first2, later2)
    for _, handed in side2:
        wait(handed)
    weigh_third()
    wait(later2)
    smooth_third()
    prolong(1, range(dims[1][0]))
    first1, later1 = begin(1)
    finish_second(*side1)
    weigh(1)
    handed1 = pass_on(1, first1)
    for slot, copy in enumerate(outer):
        copy.wait_recv()
        row = (0, dims[1][0] + 2 * REACH - 1)[slot]
        value = N[slot + 2].astype(jnp.float32)
        cells = pl.ds(REACH, dims[1][1])
        U[1][row, cells] = value.reshape(value.shape[:1] + U[1].shape[2:])
    wait(later1 + handed1)
    smooth(1)
    coarse0 = exchange(C[0], 1, plan(*dims[1], 1, True))
    edges = ((1, nx - 1, -1, 1, 2), (-1, 0, nx, 0, 3))
    early = []
    for ox, row, place, _, _ in edges:
        cells = pl.ds(REACH, ny)
        source = U[0].at[row + REACH, cells]
        early.append(send(source, U[0].at[place + REACH, cells], at(ox, 0), False))
    wait(coarse0)
    for copy in early:
        copy.wait_send()

    third = range(min(REACH, nx)), range(max(nx - REACH, 0), nx), range(nx)
    segments = []
    for rows in third:
        segments.append([i for i in rows if not any(i in segment for segment in segments)])
    messages = []
    for ox, oy, source, target, size in plan(*dims[0], REACH):
        if ox and not oy:
            shift = 1 if ox < 0 else 0
            source, target = (source[0] + shift, source[1]), (target[0] + shift, target[1])
            messages.append((ox, oy, source, target, (size[0] - 1, size[1]), V))
        elif ox:
            messages.append((ox, oy, source, target, size, V))
        else:
            for segment in segments:
                for col in range(size[1]):
                    near = beyond(target[1] + col, ny) == 1
                    place = (segment[0], source[1] + col), (segment[0], target[1] + col)
                    messages.append((0, oy) + place + ((len(segment), 1), U[0] if near else V))
    sent = len(pending)
    begin0 = []
    slim = []
    done = set()
    for fresh in segments:
        done.update(fresh)
        prolong(0, fresh)
        for ox, row, place, slot, landing in edges:
            if row in fresh:
                slim.append((place, landing, send(W.at[slot], W.at[landing], at(ox, 0))))
        ready = [m for m in messages if all(m[2][0] + i in done for i in range(m[4][0]))]
        messages = [m for m in messages if m not in ready]
        for m in ready:
            begin0.append((m, exchange(m[5], REACH, [m[:5]])[0]))
    outline = plan(*dims[0], REACH - 1)
    wait(side0)
    for m in outline:
        if m[0]:
            widen(T, S[0], 2, m[3], m[4])
    weigh(0)
    for copy in pending[:sent]:
        copy.wait_send()
    for m, copy in begin0:
        if not m[0]:
            copy.wait_recv()
            if m[5] is V:
                widen(V, U[0], REACH, m[3], m[4])

    def finish(row, result):
        middle_out[row] = result

    relax(0, finish, True)
    wait(early)
    for place, landing, copy in slim:
        copy.wait_recv()
        value = W[landing].astype(jnp.float32)
        guess = U[0][place + REACH, pl.ds(REACH, ny)]
        U[0][place + REACH, pl.ds(REACH, ny)] = guess + value.reshape(guess.shape)
    for m, copy in begin0:
        if m[0]:
            copy.wait_recv()
            widen(V, U[0], REACH, m[3], m[4])
    for copy in pending[sent:]:
        copy.wait_send()


def finishing(nx, ny, *refs):
    u, s, w0, w1, w2, q_held, p_held, middle = refs[:8]
    values, outs = refs[8:11], refs[11:15]
    q, p, o, sem = refs[15:]
    copies = []

    def store(source, target):
        copy = pltpu.make_async_copy(source, target, sem.at[len(copies)])
        copy.start()
        copies.append(copy)

    for value, out in zip(values, outs[1:]):
        store(value, out)
    for row in range(3, nx - 3):
        store(middle.at[row], outs[0].at[row])

    def finish(row, result):
        o[row] = result
        store(o.at[row], outs[0].at[row])

    def rows(held, fresh, margin):
        return lambda row: held if margin <= row < nx - margin else fresh

    q_rows, p_rows = rows(q_held, q, 1), rows(p_held, p, 2)
    held = q_held, p_held, middle
    smoothing(nx, ny, u, s, w0, w1, w2, q_rows, p_rows, finish, False, held)
    for copy in copies:
        copy.wait()


def shards(peers, *args):
    dims = [x.shape[:2] for x in args[:4]]
    sides, width = args[0].shape[2:]
    tile = (8, width)
    line = (sides // 8,) + tile
    packed = (sides, width)
    args = [x.reshape(x.shape[:2] + line) for x in args[:8]] + list(args[8:])
    for n in range(15, 18):
        if turned(args[n].shape):
            args[n] = jnp.swapaxes(args[n], 1, 2)

    args = [pltpu.with_memory_space_constraint(x, pltpu.HBM) for x in args]

    def grown(level, extra, shape, dtype=jnp.float32):
        nx, ny = dims[level]
        return (nx + extra, ny + extra) + shape, dtype

    third = dims[LAST - 1]
    columns = third[1] * peers[1]

    def rows(extra, shape, dtype=jnp.float32):
        return (third[0] + extra, columns) + shape, dtype

    results = [
        grown(0, 2 * REACH, line),
        grown(0, 4, line),
        grown(0, 4, tile),
        grown(0, 2, tile),
        grown(0, 0, tile),
        grown(0, 4, line),
        grown(0, 2, line),
        grown(0, 0, line),
    ] + [grown(level, 0, line) for level in (1, 2, 3)]
    kept = (len(Gather(peers).row), peers[1])
    scratch = (
        [grown(1, 2 * REACH, line), rows(8, line)]
        + [grown(1, 4, line), rows(6, line)]
        + [grown(0, 4, (1, width)), grown(1, 4, (1, width)), rows(6, (1, width))]
        + [grown(n, 0, (width,)) for n in range(LEVELS)]
        + [grown(1, 4, tile), rows(6, tile)]
        + [grown(1, 2, tile), rows(4, tile)]
        + [grown(1, 0, tile), rows(2, tile)]
        + [grown(1, 4, line), rows(6, line)]
        + [grown(1, 2, line), rows(4, line)]
        + [grown(0, 2 * REACH, packed, jnp.bfloat16), grown(0, 4, packed, jnp.bfloat16)]
        + [((4, dims[n][1]) + packed, jnp.bfloat16) for n in (0, 1, 1)]
        + [(x.shape, x.dtype) for x in args[12:15]]
        + [(x.shape[:2] + (2 * width, width), x.dtype) for x in args[12:15]]
        + [
            grown(1, 2, packed, jnp.bfloat16),
            rows(2, packed, jnp.bfloat16),
            grown(LAST, 2, packed, jnp.bfloat16),
        ]
        + [
            (kept + (2,) + line, jnp.float32),
            (kept + (1, width), jnp.float32),
            (kept + line, jnp.float32),
            (kept + line, jnp.float32),
            rows(0, line),
        ]
    )
    messages = message_count(dims, peers)
    anywhere = pl.BlockSpec(memory_space=pl.ANY)
    inside = pl.BlockSpec(memory_space=pltpu.VMEM)
    held = pl.pallas_call(
        partial(upward, dims, peers),
        out_shape=[pltpu.VMEM(*r) for r in results],
        in_specs=[anywhere] * 18,
        out_specs=[inside] * len(results),
        scratch_shapes=[pltpu.VMEM(*x) for x in scratch]
        + [pltpu.SMEM(x.shape, x.dtype) for x in args[15:]]
        + [
            pltpu.SemaphoreType.DMA((32,)),
            pltpu.SemaphoreType.DMA((messages,)),
            pltpu.SemaphoreType.DMA((messages,)),
        ],
        compiler_params=pltpu.CompilerParams(
            collective_id=0, has_side_effects=True, vmem_limit_bytes=40 * 2**20
        ),
    )(*args)
    nx, ny = dims[0]
    outs = pl.pallas_call(
        partial(finishing, nx, ny),
        out_shape=[jax.ShapeDtypeStruct(d + line, jnp.float32) for d in dims],
        in_specs=[inside] * len(results),
        out_specs=[anywhere] * LEVELS,
        scratch_shapes=[
            pltpu.VMEM(*grown(0, 4, line)),
            pltpu.VMEM(*grown(0, 2, line)),
            pltpu.VMEM(*grown(0, 0, line)),
            pltpu.SemaphoreType.DMA((nx + LEVELS,)),
        ],
        compiler_params=pltpu.CompilerParams(vmem_limit_bytes=16 * 2**20),
    )(*held)
    return tuple(x.reshape(x.shape[:2] + packed) for x in outs)


def solution(mesh):
    peers = (mesh.shape["gz"], mesh.shape["gy"])
    grid = P("gz", "gy")
    return jax.shard_map(
        partial(shards, peers),
        mesh=mesh,
        in_specs=(grid,) * 18,
        out_specs=(grid,) * 4,
        check_vma=False,
    )
```

```python
from functools import partial

import jax
import jax.numpy as jnp
from jax import lax
from jax.experimental import pallas as pl
from jax.experimental.pallas import tpu as pltpu
from jax.sharding import PartitionSpec as P

LEVELS = 4
REACH = 3
LAST = LEVELS - 1

upper_edge = 14.0
lower_edge = upper_edge / 8.0


def coefficients():
    centre = (upper_edge + lower_edge) / 2.0
    half_width = (upper_edge - lower_edge) / 2.0
    ratio = centre / half_width
    factor = 1.0 / ratio
    steps = []
    for _ in range(2):
        following = 1.0 / (2.0 * ratio - factor)
        steps.append((following * factor, 2.0 * following / half_width))
        factor = following
    (a1, b1), (a2, b2) = steps
    first = 1.0 / centre
    return {
        "own1": first * (a1 + b1 * centre),
        "side1": first * b1,
        "start2": first * (1.0 - a1 * b2 / b1),
        "own2": 1.0 + a2 + b2 / b1,
        "side2": b2,
    }


def beyond(index, length):
    return max(-index, index - length + 1, 0)


def plan(nx, ny, reach, box=False):
    def width(row):
        return reach if box else reach - beyond(row, nx)

    out = []
    far_x, far_y = -(-reach // nx), -(-reach // ny)
    for ox in range(-far_x, far_x + 1):
        for oy in range(-far_y, far_y + 1):
            if ox == 0 and oy == 0:
                continue
            runs = []
            for row in range(max(-ox * nx, -reach), min((1 - ox) * nx, nx + reach)):
                low = max(-oy * ny, -width(row))
                high = min((1 - oy) * ny, ny + width(row))
                if low >= high:
                    continue
                if runs and runs[-1][2:] == (low, high) and runs[-1][1] == row:
                    runs[-1] = (runs[-1][0], row + 1, low, high)
                else:
                    runs.append((row, row + 1, low, high))
            for top, end, low, high in runs:
                out.append(
                    (ox, oy, (top + ox * nx, low + oy * ny), (top, low), (end - top, high - low))
                )
    out.sort(key=lambda m: (-abs(m[0]), -abs(m[1]), m))
    return out


class Gather:
    def __init__(self, peers):
        self.size = peers
        rows = {x % peers[0]: abs(x) for x in (4, -4, 3, -3, 2, -2, 1, -1, 0)}
        self.far = {x: min(x, peers[0] - x) for x in rows}
        self.row = {x: k for k, x in enumerate(sorted(rows))}

    def around(self, reach):
        cells = []
        for x in range(-reach - 1, reach + 2):
            for y in range(-reach - 1, reach + 2):
                far = max(abs(x) - 1, 0) + max(abs(y) - 1, 0)
                cell = (x % self.size[0], y % self.size[1])
                if far <= reach and cell not in cells:
                    cells.append(cell)
        return cells

    def messages(self):
        out = []
        for x in self.row:
            for y in range(0, self.size[1], 2):
                if x or y:
                    out.append((-self.far[x] - min(y, self.size[1] - y), x, y, self.far[x] <= 3))
        out.sort()
        return [m[1:] for m in out]


def modulo(value, size):
    if size & (size - 1) == 0:
        return jnp.bitwise_and(value, size - 1)
    return lax.rem(value, size)


def quotient(value, size):
    if size & (size - 1) == 0:
        return jnp.right_shift(value, size.bit_length() - 1)
    return lax.div(value, size)


class Counter:
    def __init__(self):
        self.used = 0

    def take(self):
        self.used += 1
        return self.used - 1


def corners(nx, ny):
    out = []
    for ox in (1, -1):
        for far in range(1, REACH):
            target, source = (-far, nx - far) if ox > 0 else (nx - 1 + far, far - 1)
            out.append((ox, target, source, REACH - far))
    return out


def straight(nx, ny):
    near, rest = [], []
    for ox, oy, source, target, size in plan(nx, ny, REACH):
        if ox and oy:
            continue
        if not ox:
            rest.append((ox, oy, source, target, size))
            continue
        for row in range(size[0]):
            far = beyond(target[0] + row, nx)
            group = near if far < REACH else rest
            m = (ox, oy, (source[0] + row, source[1]), (target[0] + row, target[1]), (1, size[1]))
            group.append(m)
    near.sort(key=lambda m: beyond(m[3][0], nx))
    rest.sort(key=lambda m: -abs(m[0]))
    return near, rest


def slab(nx, reach, peers):
    far = -(-reach // nx)
    out = []
    for ox in range(-far, far + 1):
        for oy in range(0, peers[1], 2):
            top, end = max(-ox * nx, -reach), min((1 - ox) * nx, nx + reach)
            if (ox or oy) and top < end:
                out.append((ox, oy, top + ox * nx, top, end - top))
    out.sort(key=lambda m: (abs(m[0]) + min(m[1], peers[1] - m[1]), m))
    return out


def message_count(dims, peers):
    total = 14 + 2 * sum(1 + m[-1] for m in Gather(peers).messages())
    third = dims[LAST - 1][0]
    total += 2 * (1 + len(slab(third, REACH + 1, peers)) + 2 * len(slab(third, REACH, peers)) + 2)
    for level, (nx, ny) in enumerate(dims[: LAST - 1]):
        total += len(plan(nx, ny, REACH)) + 2 * len(plan(nx, ny, REACH - 1))
        if level:
            total += len(plan(nx, ny, 1, True)) + 4 * REACH
        else:
            total += 6 * REACH
    return total


def partners(dims, peers):
    found = set()
    for nx, ny in dims[: LAST - 1]:
        for m in plan(nx, ny, REACH) + plan(nx, ny, 1, True):
            found.add((m[0] % peers[0], m[1] % peers[1]))
            found.add((-m[0] % peers[0], -m[1] % peers[1]))
    around = [m[:2] for m in slab(dims[LAST - 1][0], REACH + 1, peers)]
    for x, y in around + [m[:2] for m in Gather(peers).messages()]:
        found.add((x % peers[0], y % peers[1]))
        found.add((-x % peers[0], -y % peers[1]))
    return sorted(found)


def turned(shape):
    return shape[1] > shape[2]


def beside(centre, above, below):
    middle = centre[1:-1]
    line = middle.shape[-1]
    total = centre[:-2] + centre[2:]
    for other in (above, below):
        if other is not None:
            total = total + other
    return total + (pltpu.roll(middle, 1, 3) + pltpu.roll(middle, line - 1, 3))


def smoothing(nx, ny, u, s, w0, w1, w2, q, p, finish, middle=None, held=None):
    k = coefficients()

    def share(row, margin):
        if middle is None:
            return "all"
        inside = margin <= row < nx - margin
        edge = row in (margin - 1, nx - margin) and nx > 2 * REACH
        if middle:
            return "all" if inside else "inner" if edge else None
        return None if inside else "outer" if edge else "all"

    def around(ref, row, pad, cells, part, margin):
        sides = []
        for other in (row - 1, row + 1):
            outer = (other < row) == (row == margin - 1)
            wanted = part == "all" or (part == "outer") == outer
            sides.append(ref(other)[other + pad, cells] if wanted else None)
        return [x for x in sides if x is not None][0] if part == "outer" else sides

    def start(row, part):
        w = 2 - beyond(row, nx)
        count = ny + 2 * w
        cells, inner = pl.ds(2 - w, count), pl.ds(3 - w, count)
        others = around(lambda _: u, row, 3, inner, part, 1)
        if part == "outer":
            q(row)[row + 2, cells] = held[0][row + 2, cells] + others
            return
        near = beside(u[row + 3, pl.ds(2 - w, count + 2)], *others)
        weight = w0[row + 2, cells][:, None]
        q(row)[row + 2, cells] = (s[row + 2, cells] - weight * u[row + 3, inner]) + near

    def second(row, part):
        w = 1 - beyond(row, nx)
        count = ny + 2 * w
        cells, inner = pl.ds(1 - w, count), pl.ds(2 - w, count)
        others = around(q, row, 2, inner, part, 2)
        if part == "outer":
            p(row)[row + 1, cells] = held[1][row + 1, cells] + k["side1"] * others
            return
        near = beside(q(row)[row + 2, pl.ds(1 - w, count + 2)], *others)
        weight = w1[row + 1, cells][:, None]
        p(row)[row + 1, cells] = weight * q(row)[row + 2, inner] + k["side1"] * near

    def third(row, part):
        cells = pl.ds(1, ny)
        others = around(p, row, 1, cells, part, 3)
        if part == "outer":
            finish(row, held[2][row] + k["side2"] * others)
            return
        near = beside(p(row)[row + 1, pl.ds(0, ny + 2)], *others)
        begin = u[row + 3, pl.ds(3, ny)] + k["start2"] * q(row)[row + 2, pl.ds(2, ny)]
        finish(row, (begin + w2[row][:, None] * p(row)[row + 1, cells]) + k["side2"] * near)

    for row in range(-2, nx + 6):
        if row < nx + 2 and share(row, 1):
            start(row, share(row, 1))
        if -1 <= row - 2 < nx + 1 and share(row - 2, 2):
            second(row - 2, share(row - 2, 2))
        if 0 <= row - 4 < nx and share(row - 4, 3):
            third(row - 4, share(row - 4, 3))


def upward(dims, peers, *refs):
    refs = list(refs)

    def take(count):
        got = refs[:count]
        del refs[:count]
        return got

    sources, guesses, shifts = take(4), take(4), take(4)
    blocks, link_inputs = take(3), take(3)
    start_out, source_out, w0_out, w1_out, w2_out, q_out, p_out, middle_out = take(8)
    outs = [None] + take(3)
    U, S = [start_out] + take(2), [source_out] + take(2)
    D, H = take(3), take(4)
    W0, W1, W2 = [w0_out] + take(2), [w1_out] + take(2), [w2_out] + take(2)
    Q, PD = [q_out] + take(2), [p_out] + take(2)
    V, T, W, N, M = take(5)
    B, BT, C = take(3), take(3), take(3)
    K, DK, QK, PK = take(4)
    R = refs.pop(0)
    links = take(3)
    local_sem, send_sem, recv_sem = take(3)
    gz, gy = lax.axis_index("gz"), lax.axis_index("gy")
    k = coefficients()

    side = lax.rem(gy, 2)

    def at(ox, oy):
        oy = oy % peers[1] if isinstance(oy, int) else oy + peers[1]
        return (lax.rem(gz + (ox % peers[0]), peers[0]), lax.rem(gy + oy, peers[1]))

    partner = at(0, 1 - 2 * side)

    barrier = pltpu.get_barrier_semaphore()
    company = partners(dims, peers)
    for ox, oy in company:
        pl.semaphore_signal(barrier, inc=1, device_id=at(ox, oy), device_id_type=pl.DeviceIdType.MESH)

    local = Counter()

    def fetch(source, target):
        copy = pltpu.make_async_copy(source, target, local_sem.at[local.take()])
        copy.start()
        return copy

    gather = Gather(peers)
    loads = [None] * LEVELS
    loads[LAST] = [
        fetch(guesses[LAST].at[0, 0], K.at[gather.row[0], gy, 0]),
        fetch(sources[LAST].at[0, 0], K.at[gather.row[0], gy, 1]),
        fetch(shifts[LAST], H[LAST]),
    ]

    def own(ref, level, reach):
        nx, ny = dims[level]
        return ref.at[pl.ds(reach, nx), pl.ds(reach, ny)]

    third = LAST - 1
    mine = pl.ds(gy * dims[third][1], dims[third][1])
    for level in reversed(range(LAST)):
        loads[level] = [fetch(shifts[level], H[level])]
        if level == third:
            rows = dims[third][0]
            loads[level].append(fetch(sources[level], S[level].at[pl.ds(REACH, rows), mine]))
            loads[level].append(fetch(guesses[level], U[level].at[pl.ds(REACH + 1, rows), mine]))
        else:
            loads[level].append(fetch(sources[level], own(S[level], level, REACH - 1)))
            loads[level].append(fetch(guesses[level], own(U[level], level, REACH)))
    for level in reversed(range(LAST)):
        loads[level].append(fetch(link_inputs[level], links[level]))
    block_loads = [None] * LAST
    for level in reversed(range(LAST)):
        block_loads[level] = fetch(blocks[level], B[level])

    for copy in loads[LAST]:
        copy.wait()
    DK[gather.row[0], gy] = 6.0 + H[LAST][0]

    pl.semaphore_wait(barrier, len(company))

    counter = Counter()
    pending = []

    def send(source, target, device, later=True):
        index = counter.take()
        copy = pltpu.make_async_remote_copy(
            src_ref=source,
            dst_ref=target,
            send_sem=send_sem.at[index],
            recv_sem=recv_sem.at[index],
            device_id=device,
            device_id_type=pl.DeviceIdType.MESH,
        )
        copy.start()
        if later:
            pending.append(copy)
        return copy

    def rectangle(ref, corner, size, pad):
        return ref.at[pl.ds(corner[0] + pad, size[0]), pl.ds(corner[1] + pad, size[1])]

    def exchange(ref, pad, messages):
        return [
            send(rectangle(ref, source, size, pad), rectangle(ref, target, size, pad), at(ox, oy))
            for ox, oy, source, target, size in messages
        ]

    def share(row, column, whole, device):
        cell = (row, column)
        if whole:
            return [
                send(K.at[cell], K.at[cell], device),
                send(DK.at[cell], DK.at[cell], device),
            ]
        return [send(K.at[cell].at[0], K.at[cell].at[0], device)]

    last = []
    for x, y, whole in gather.messages():
        source, target = (gather.row[0], gy), (gather.row[x], gy)
        copies = []
        if whole:
            copies.append(send(K.at[source], K.at[target], at(-x, -y)))
            copies.append(send(DK.at[source], DK.at[target], at(-x, -y)))
        else:
            copies.append(send(K.at[source].at[0], K.at[target].at[0], at(-x, -y)))
        last.append((gather.row[x], lax.rem(gy + y, peers[1]), whole, copies))
    handed = share(gather.row[0], gy, True, partner)

    def diagonals(level):
        nx, ny = dims[level]
        for copy in loads[level]:
            copy.wait()
        for i in range(nx):
            for j in range(ny):
                d = 6.0 + H[level][i, pl.ds(j, 1)]
                if level == third:
                    D[level][i + REACH, gy * ny + j] = d
                else:
                    D[level][i + 2, j + 2] = d

    def sides(level, narrow=None):
        messages = plan(*dims[level], REACH - 1)
        copies = []
        for m in messages:
            ref = S[level] if narrow is None or m[0] == 0 else narrow
            copies += exchange(ref, 2, [m])
        return copies + exchange(D[level], 2, messages)

    def sides_second():
        nx, ny = dims[1]
        s = S[1]
        copies, near, thin = [], [], []
        for slot, row in enumerate((nx - 2, 1)):
            value = s[row + 2, pl.ds(2, ny)]
            M[slot] = value.reshape(value.shape[:1] + M.shape[2:]).astype(jnp.bfloat16)
        for slot, (ox, source, target) in enumerate(((1, nx - 1, -1), (-1, 0, nx))):
            cells = pl.ds(2, ny)
            near.append((target, send(s.at[source + 2, cells], s.at[target + 2, cells], at(ox, 0))))
            start, stop = side * (ny - 1) + 2, side * (-1 - ny) + ny + 2
            corner = s.at[source + 2, pl.ds(start, 1)], s.at[target + 2, pl.ds(stop, 1)]
            copies.append(send(*corner, at(ox, 2 * side - 1)))
            thin.append(send(M.at[slot], M.at[slot + 2], at(ox, 0)))
        messages = plan(nx, ny, REACH - 1)
        copies += exchange(s, 2, [m for m in messages if not m[0]])
        return copies + exchange(D[1], 2, messages), near, thin

    def finish_second(copies, near, thin):
        nx, ny = dims[1]
        s = S[1]
        handed = []
        for target, copy in near:
            copy.wait_recv()
            start = (1 - side) * (ny - 1) + 2
            stop = (1 - side) * (-1 - ny) + ny + 2
            corner = s.at[target + 2, pl.ds(start, 1)], s.at[target + 2, pl.ds(stop, 1)]
            handed.append(send(*corner, partner))
        for slot, copy in enumerate(thin):
            copy.wait_recv()
            value = M[slot + 2].astype(jnp.float32)
            row = (0, nx + 3)[slot]
            s[row, pl.ds(2, ny)] = value.reshape(value.shape[:1] + s.shape[2:])
        wait(copies + handed)

    def weigh(level):
        nx, ny = dims[level]
        for row in range(-2, nx + 2):
            w = 2 - beyond(row, nx)
            for col in range(-w, ny + w):
                d = jnp.broadcast_to(D[level][row + 2, col + 2], W0[level].shape[2:])
                W0[level][row + 2, col + 2] = d
                far = beyond(row, nx) + beyond(col, ny)
                if far <= 1:
                    W1[level][row + 1, col + 1] = k["own1"] - k["side1"] * d
                if far == 0:
                    W2[level][row, col] = k["own2"] - k["side2"] * d

    def spread(ref, reach):
        nx = dims[third][0]
        whole = pl.ds(reach, nx)
        copies = []
        for ox, oy, source, target, count in slab(nx, REACH + 1 if ref is U[third] else REACH, peers):
            start, stop = pl.ds(source + reach, count), pl.ds(target + reach, count)
            column = lax.rem(gy + peers[1] - oy, peers[1]) * dims[third][1]
            copy = send(ref.at[start, mine], ref.at[stop, mine], at(ox, oy))
            copies.append((stop, pl.ds(column, dims[third][1]), copy))
        return copies, [send(ref.at[whole, mine], ref.at[whole, mine], partner)]

    def hand(ref, copies, handed):
        for rows, columns, copy in copies:
            copy.wait_recv()
            handed.append(send(ref.at[rows, columns], ref.at[rows, columns], partner))

    def weigh_third():
        nx, columns = dims[third][0], D[third].shape[1]
        for row in range(-REACH, nx + REACH):
            for col in range(columns):
                d = jnp.broadcast_to(D[third][row + REACH, col], W0[third].shape[2:])
                W0[third][row + REACH, col] = d
                if -2 <= row < nx + 2:
                    W1[third][row + 2, col] = k["own1"] - k["side1"] * d
                if -1 <= row < nx + 1:
                    W2[third][row + 1, col] = k["own2"] - k["side2"] * d

    def smooth_third():
        nx, ny = dims[third]
        u, s, q, p = U[third], S[third], Q[third], PD[third]

        def near(ref, row):
            middle = ref[row]
            ring = jnp.concatenate([middle[-1:], middle, middle[:1]], axis=0)
            return middle, beside(ring, ref[row - 1], ref[row + 1])

        for row in range(-3, nx + 3):
            middle, total = near(u, row + 4)
            q[row + 3] = (s[row + 3] - W0[third][row + 3][:, None] * middle) + total
        for row in range(-2, nx + 2):
            middle, total = near(q, row + 3)
            p[row + 2] = W1[third][row + 2][:, None] * middle + k["side1"] * total
        for row in range(-1, nx + 1):
            middle, total = near(p, row + 2)
            begin = u[row + 4] + k["start2"] * q[row + 3]
            result = begin + W2[third][row + 1][:, None] * middle + k["side2"] * total
            lines = result.reshape(result.shape[:1] + C[third - 1].shape[2:])
            C[third - 1][row + 1] = lines.astype(jnp.bfloat16)
            if 0 <= row < nx:
                R[row] = result
        for row in range(nx):
            outs[third][row] = R[row, mine]

    def turn(level):
        nx, ny = dims[level]
        block_loads[level].wait()
        line = B[level].shape[-1]

        def body(i, carry):
            for j in range(ny):
                for part in range(2):
                    BT[level][i, j, pl.ds(part * line, line)] = B[level][i, j, part].T
            return carry

        lax.fori_loop(0, nx, body, 0)

    def relax(level, finish, middle=None):
        weights = W0[level], W1[level], W2[level]
        q, p = Q[level], PD[level]
        smoothing(*dims[level], U[level], S[level], *weights, lambda r: q, lambda r: p, finish, middle)

    def smooth(level):
        nx, ny = dims[level]

        def finish(row, result):
            outs[level][row] = result
            lines = result.reshape(result.shape[:1] + C[level - 1].shape[2:])
            C[level - 1][row + 1, pl.ds(1, ny)] = lines.astype(jnp.bfloat16)

        relax(level, finish)

    def smooth_last():
        column = [lax.rem(gy + y, peers[1]) for y in range(peers[1])]

        def place(x, y):
            return gather.row[x % peers[0]], column[y % peers[1]]

        def near(ref, x, y):
            middle = ref[place(x, y)]
            total = ref[place(x, y - 1)] + ref[place(x, y + 1)]
            total = total + (ref[place(x - 1, y)] + ref[place(x + 1, y)])
            line = middle.shape[-1]
            return middle, total + (pltpu.roll(middle, 1, 2) + pltpu.roll(middle, line - 1, 2))

        for x, y in gather.around(2):
            middle, total = near(K.at[:, :, 0], x, y)
            QK[place(x, y)] = (K[place(x, y) + (1,)] - DK[place(x, y)] * middle) + total
        for x, y in gather.around(1):
            middle, total = near(QK, x, y)
            weight = k["own1"] - k["side1"] * DK[place(x, y)]
            PK[place(x, y)] = weight * middle + k["side1"] * total
        for x in range(-1, 2):
            for y in range(-1, 2):
                middle, total = near(PK, x, y)
                weight = k["own2"] - k["side2"] * DK[place(x, y)]
                begin = K[place(x, y) + (0,)] + k["start2"] * QK[place(x, y)]
                result = begin + weight * middle + k["side2"] * total
                if x == 0 and y == 0:
                    outs[LAST][0, 0] = result
                C[LAST - 1][x + 1, y + 1] = result.reshape(C[LAST - 1].shape[2:]).astype(jnp.bfloat16)

    outer = []

    def begin(level):
        nx, ny = dims[level]
        u = U[level]
        near, rest = straight(nx, ny)
        first = list(zip(near, exchange(u, REACH, near)))
        later = []
        for ox, target, source, width in corners(nx, ny):
            start = side * (ny - width) + REACH
            stop = side * (-width - ny) + ny + REACH
            later.append(
                send(
                    u.at[source + REACH, pl.ds(start, width)],
                    u.at[target + REACH, pl.ds(stop, width)],
                    at(ox, 2 * side - 1),
                )
            )
        if level == 1:
            for slot, ox in enumerate((1, -1)):
                outer.append(send(N.at[slot], N.at[slot + 2], at(ox, 0)))
            rest = [m for m in rest if not m[0]]
        later += exchange(u, REACH, rest)
        return first, later

    def pass_on(level, first):
        nx, ny = dims[level]
        u = U[level]
        widths = {target: width for _, target, _, width in corners(nx, ny)}
        copies = []
        for m, copy in first:
            copy.wait_recv()
            row, width = m[3][0], widths[m[3][0]]
            start = (1 - side) * (ny - width) + REACH
            stop = (1 - side) * (-width - ny) + ny + REACH
            copies.append(
                send(
                    u.at[row + REACH, pl.ds(start, width)],
                    u.at[row + REACH, pl.ds(stop, width)],
                    partner,
                )
            )
        return copies

    def prolong(level, rows):
        nx, ny = dims[level]
        cx, cy = dims[level + 1]
        full = (cx * peers[0], cy * peers[1])
        lift_x = full[0] + 1 - gz * cx
        lift_y = full[1] + 1 - gy * cy

        def pick(i, j, side):
            if turned((nx, ny, 2)):
                link = links[level][i, side, j]
            else:
                link = links[level][i, j, side]
            row = modulo(quotient(link, full[1]) + lift_x, full[0])
            col = modulo(link, full[1])
            if level + 1 != third:
                col = jnp.minimum(modulo(col + lift_y, full[1]), cy + 1)
            return C[level][jnp.minimum(row, cx + 1), col]

        for i in rows:
            for j in range(ny):
                picked = jnp.concatenate([pick(i, j, 0), pick(i, j, 1)], axis=1)
                sums = lax.dot_general(
                    picked, BT[level][i, j], (((1,), (0,)), ((), ())), preferred_element_type=jnp.float32
                )
                place = i + REACH, j + REACH
                if level == third:
                    place = i + REACH + 1, gy * ny + j
                u = U[level][place]
                u = u + sums.reshape(u.shape)
                U[level][place] = u
                if level == 0:
                    V[i + REACH, j + REACH] = u.reshape(sums.shape).astype(jnp.bfloat16)
                    if i == 0:
                        W[0, j] = sums.astype(jnp.bfloat16)
                    if i == nx - 1:
                        W[1, j] = sums.astype(jnp.bfloat16)
                if level == 1:
                    for slot, row in enumerate((nx - REACH, REACH - 1)):
                        if i == row:
                            N[slot, j] = u.reshape(sums.shape).astype(jnp.bfloat16)

    def widen(source, target, pad, corner, size):
        for row in range(corner[0] + pad, corner[0] + pad + size[0]):
            cells = pl.ds(corner[1] + pad, size[1])
            value = source[row, cells].astype(jnp.float32)
            target[row, cells] = value.reshape(value.shape[:1] + target.shape[2:])

    diagonals(2)
    diagonals(1)
    diagonals(0)
    nx, ny = dims[0]
    for i in range(nx):
        value = S[0][i + 2, pl.ds(2, ny)]
        T[i + 2, pl.ds(2, ny)] = value.reshape(value.shape[:1] + T.shape[2:]).astype(jnp.bfloat16)
    for level in reversed(range(LAST)):
        turn(level)

    def wait(copies):
        for copy in copies:
            copy.wait_recv()

    for row, column, whole, copies in last:
        wait(copies)
        handed += share(row, column, whole, partner)
    side2 = spread(S[third], REACH), spread(D[third], REACH)
    wait(handed)
    smooth_last()
    prolong(2, range(dims[2][0]))
    first2, later2 = spread(U[third], REACH + 1)
    side1 = sides_second()
    side0 = sides(0, T)
    for ref, (copies, handed) in zip((S[third], D[third]), side2):
        hand(ref, copies, handed)
    hand(U[third], first2, later2)
    for _, handed in side2:
        wait(handed)
    weigh_third()
    wait(later2)
    smooth_third()
    prolong(1, range(dims[1][0]))
    first1, later1 = begin(1)
    finish_second(*side1)
    weigh(1)
    handed1 = pass_on(1, first1)
    for slot, copy in enumerate(outer):
        copy.wait_recv()
        row = (0, dims[1][0] + 2 * REACH - 1)[slot]
        value = N[slot + 2].astype(jnp.float32)
        cells = pl.ds(REACH, dims[1][1])
        U[1][row, cells] = value.reshape(value.shape[:1] + U[1].shape[2:])
    wait(later1 + handed1)
    smooth(1)
    coarse0 = exchange(C[0], 1, plan(*dims[1], 1, True))
    edges = ((1, nx - 1, -1, 1, 2), (-1, 0, nx, 0, 3))
    early = []
    for ox, row, place, _, _ in edges:
        cells = pl.ds(REACH, ny)
        source = U[0].at[row + REACH, cells]
        early.append(send(source, U[0].at[place + REACH, cells], at(ox, 0), False))
    wait(coarse0)
    for copy in early:
        copy.wait_send()

    third = range(min(REACH, nx)), range(max(nx - REACH, 0), nx), range(nx)
    segments = []
    for rows in third:
        segments.append([i for i in rows if not any(i in segment for segment in segments)])
    messages = []
    for ox, oy, source, target, size in plan(*dims[0], REACH):
        if ox and not oy:
            shift = 1 if ox < 0 else 0
            source, target = (source[0] + shift, source[1]), (target[0] + shift, target[1])
            messages.append((ox, oy, source, target, (size[0] - 1, size[1]), V))
        elif ox:
            messages.append((ox, oy, source, target, size, V))
        else:
            for segment in segments:
                for col in range(size[1]):
                    near = beyond(target[1] + col, ny) == 1
                    place = (segment[0], source[1] + col), (segment[0], target[1] + col)
                    messages.append((0, oy) + place + ((len(segment), 1), U[0] if near else V))
    sent = len(pending)
    begin0 = []
    slim = []
    done = set()
    for fresh in segments:
        done.update(fresh)
        prolong(0, fresh)
        for ox, row, place, slot, landing in edges:
            if row in fresh:
                slim.append((place, landing, send(W.at[slot], W.at[landing], at(ox, 0))))
        ready = [m for m in messages if all(m[2][0] + i in done for i in range(m[4][0]))]
        messages = [m for m in messages if m not in ready]
        for m in ready:
            begin0.append((m, exchange(m[5], REACH, [m[:5]])[0]))
    outline = plan(*dims[0], REACH - 1)
    wait(side0)
    for m in outline:
        if m[0]:
            widen(T, S[0], 2, m[3], m[4])
    weigh(0)
    for copy in pending[:sent]:
        copy.wait_send()
    for m, copy in begin0:
        if not m[0]:
            copy.wait_recv()
            if m[5] is V:
                widen(V, U[0], REACH, m[3], m[4])

    def finish(row, result):
        middle_out[row] = result

    relax(0, finish, True)
    wait(early)
    for place, landing, copy in slim:
        copy.wait_recv()
        value = W[landing].astype(jnp.float32)
        guess = U[0][place + REACH, pl.ds(REACH, ny)]
        U[0][place + REACH, pl.ds(REACH, ny)] = guess + value.reshape(guess.shape)
    for m, copy in begin0:
        if m[0]:
            copy.wait_recv()
            widen(V, U[0], REACH, m[3], m[4])
    for copy in pending[sent:]:
        copy.wait_send()


def finishing(nx, ny, *refs):
    u, s, w0, w1, w2, q_held, p_held, middle = refs[:8]
    values, outs = refs[8:11], refs[11:15]
    q, p, o, sem = refs[15:]
    copies = []

    def store(source, target):
        copy = pltpu.make_async_copy(source, target, sem.at[len(copies)])
        copy.start()
        copies.append(copy)

    for value, out in zip(values, outs[1:]):
        store(value, out)
    for row in range(3, nx - 3):
        store(middle.at[row], outs[0].at[row])

    def finish(row, result):
        o[row] = result
        store(o.at[row], outs[0].at[row])

    def rows(held, fresh, margin):
        return lambda row: held if margin <= row < nx - margin else fresh

    q_rows, p_rows = rows(q_held, q, 1), rows(p_held, p, 2)
    held = q_held, p_held, middle
    smoothing(nx, ny, u, s, w0, w1, w2, q_rows, p_rows, finish, False, held)
    for copy in copies:
        copy.wait()


def shards(peers, *args):
    dims = [x.shape[:2] for x in args[:4]]
    sides, width = args[0].shape[2:]
    tile = (8, width)
    line = (sides // 8,) + tile
    packed = (sides, width)
    args = [x.reshape(x.shape[:2] + line) for x in args[:8]] + list(args[8:])
    for n in range(15, 18):
        if turned(args[n].shape):
            args[n] = jnp.swapaxes(args[n], 1, 2)

    args = [pltpu.with_memory_space_constraint(x, pltpu.HBM) for x in args]

    def grown(level, extra, shape, dtype=jnp.float32):
        nx, ny = dims[level]
        return (nx + extra, ny + extra) + shape, dtype

    third = dims[LAST - 1]
    columns = third[1] * peers[1]

    def rows(extra, shape, dtype=jnp.float32):
        return (third[0] + extra, columns) + shape, dtype

    results = [
        grown(0, 2 * REACH, line),
        grown(0, 4, line),
        grown(0, 4, tile),
        grown(0, 2, tile),
        grown(0, 0, tile),
        grown(0, 4, line),
        grown(0, 2, line),
        grown(0, 0, line),
    ] + [grown(level, 0, line) for level in (1, 2, 3)]
    kept = (len(Gather(peers).row), peers[1])
    scratch = (
        [grown(1, 2 * REACH, line), rows(8, line)]
        + [grown(1, 4, line), rows(6, line)]
        + [grown(0, 4, (1, width)), grown(1, 4, (1, width)), rows(6, (1, width))]
        + [grown(n, 0, (width,)) for n in range(LEVELS)]
        + [grown(1, 4, tile), rows(6, tile)]
        + [grown(1, 2, tile), rows(4, tile)]
        + [grown(1, 0, tile), rows(2, tile)]
        + [grown(1, 4, line), rows(6, line)]
        + [grown(1, 2, line), rows(4, line)]
        + [grown(0, 2 * REACH, packed, jnp.bfloat16), grown(0, 4, packed, jnp.bfloat16)]
        + [((4, dims[n][1]) + packed, jnp.bfloat16) for n in (0, 1, 1)]
        + [(x.shape, x.dtype) for x in args[12:15]]
        + [(x.shape[:2] + (2 * width, width), x.dtype) for x in args[12:15]]
        + [
            grown(1, 2, packed, jnp.bfloat16),
            rows(2, packed, jnp.bfloat16),
            grown(LAST, 2, packed, jnp.bfloat16),
        ]
        + [
            (kept + (2,) + line, jnp.float32),
            (kept + (1, width), jnp.float32),
            (kept + line, jnp.float32),
            (kept + line, jnp.float32),
            rows(0, line),
        ]
    )
    messages = message_count(dims, peers)
    anywhere = pl.BlockSpec(memory_space=pl.ANY)
    inside = pl.BlockSpec(memory_space=pltpu.VMEM)
    held = pl.pallas_call(
        partial(upward, dims, peers),
        out_shape=[pltpu.VMEM(*r) for r in results],
        in_specs=[anywhere] * 18,
        out_specs=[inside] * len(results),
        scratch_shapes=[pltpu.VMEM(*x) for x in scratch]
        + [pltpu.SMEM(x.shape, x.dtype) for x in args[15:]]
        + [
            pltpu.SemaphoreType.DMA((32,)),
            pltpu.SemaphoreType.DMA((messages,)),
            pltpu.SemaphoreType.DMA((messages,)),
        ],
        compiler_params=pltpu.CompilerParams(
            collective_id=0, has_side_effects=True, vmem_limit_bytes=40 * 2**20
        ),
    )(*args)
    nx, ny = dims[0]
    outs = pl.pallas_call(
        partial(finishing, nx, ny),
        out_shape=[jax.ShapeDtypeStruct(d + line, jnp.float32) for d in dims],
        in_specs=[inside] * len(results),
        out_specs=[anywhere] * LEVELS,
        scratch_shapes=[
            pltpu.VMEM(*grown(0, 4, line)),
            pltpu.VMEM(*grown(0, 2, line)),
            pltpu.VMEM(*grown(0, 0, line)),
            pltpu.SemaphoreType.DMA((nx + LEVELS,)),
        ],
        compiler_params=pltpu.CompilerParams(vmem_limit_bytes=16 * 2**20),
    )(*held)
    return tuple(x.reshape(x.shape[:2] + packed) for x in outs)


def solution(mesh):
    peers = (mesh.shape["gz"], mesh.shape["gy"])
    grid = P("gz", "gy")
    return jax.shard_map(
        partial(shards, peers),
        mesh=mesh,
        in_specs=(grid,) * 18,
        out_specs=(grid,) * 4,
        check_vma=False,
    )
```
